32 devices in a mesh: sys: 2 (over x), col: 4 (over z), seg: 4 (over y, core).
Axes of the slice: x: 2, y: 2, z: 4, core: 2. Of those that a mesh axis runs over, the one named last changes fastest.
Arguments:
- positions: bfloat16 [32768, 256], P(('sys', 'seg', 'col')), parts along dimension 0
- charges: float32 [32768], P(('sys', 'seg', 'col')), parts along dimension 0
Outputs:
- output 1: float32 [32768, 256], P(('sys', 'seg', 'col')), parts along dimension 0
- output 2: float32 [2], P('sys'), parts along dimension 0
There are 2 independent parts. The reference program is written for one: setup_inputs(seed, part) draws one part's arguments, and reference() takes and returns one part's arrays. A program takes and returns all parts, laid end to end along the dimension named above; each array names one.
All inputs are finite; a program needn't handle non-finite values.
Results may differ from the reference program's by a relative error of at most 0.001.
Values are sent between devices in bfloat16 or wider.
A program may use at most 1 GiB of HBM per device.

```python
import jax
import jax.numpy as jnp
from jax import lax

PARTICLES = 16384
FEAT_DIM = 256
ROW_BLOCK = min(PARTICLES, 256)
BLOCK_COUNT = PARTICLES // ROW_BLOCK
INV_LEN2 = 1.0 / FEAT_DIM
CHARGE_SCALE = (2.0 * FEAT_DIM) ** 0.5 * PARTICLES ** -0.25


def setup_inputs(seed: int = 0, part: int = 0) -> dict:
    base_key = jax.random.fold_in(jax.random.key(seed), part)
    key_pos, key_charge = jax.random.split(base_key)
    positions = jax.random.normal(key_pos, (PARTICLES, FEAT_DIM), jnp.float32).astype(jnp.bfloat16)
    charges = CHARGE_SCALE * jax.random.normal(key_charge, (PARTICLES,), jnp.float32)
    return {'positions': positions, 'charges': charges}


def reference(positions, charges):
    pos_wide = positions.astype(jnp.float32)
    sq_norm = jnp.sum(pos_wide * pos_wide, axis=1)
    all_pos = jnp.arange(PARTICLES)

    def one_block(blk_index):
        row_start = blk_index * ROW_BLOCK
        x_rows = lax.dynamic_slice_in_dim(positions, row_start, ROW_BLOCK, 0)
        q_rows = lax.dynamic_slice_in_dim(charges, row_start, ROW_BLOCK, 0)
        s_rows = lax.dynamic_slice_in_dim(sq_norm, row_start, ROW_BLOCK, 0)
        dot_prod = jnp.dot(x_rows, positions.T, preferred_element_type=jnp.float32)
        sq_dist = jnp.maximum(s_rows[:, None] + sq_norm[None, :] - 2.0 * dot_prod, 0.0)
        weights = q_rows[:, None] * charges[None, :] * jnp.exp(-0.5 * INV_LEN2 * sq_dist)
        row_ids = row_start + jnp.arange(ROW_BLOCK)
        weights = jnp.where(row_ids[:, None] == all_pos[None, :], 0.0, weights)
        pulled = jnp.dot(weights.astype(jnp.bfloat16), positions, preferred_element_type=jnp.float32)
        forces = (jnp.sum(weights, axis=1)[:, None] * x_rows.astype(jnp.float32) - pulled) * INV_LEN2
        return forces, jnp.sum(weights)

    forces, energies = lax.map(one_block, jnp.arange(BLOCK_COUNT))
    return forces.reshape(PARTICLES, FEAT_DIM), (0.5 * jnp.sum(energies)).reshape(1)
```

```python
import functools
import math

import jax
import jax.numpy as jnp
from jax import lax
from jax.experimental import pallas as pl
from jax.experimental.pallas import tpu as pltpu
from jax.sharding import PartitionSpec as P

ROW_AXES = ('sys', 'seg', 'col')
MESH = pl.DeviceIdType.MESH
NT = (((1,), (1,)), ((), ()))
PARTS = 4
LANES = 128


def pair_kernel(x_hbm, q_ref, out_ref, e_ref, xs, aq, es, a_col, q_col, force, row_sum,
                load_sem, recv_sem, aq_recv, e_recv, send_sem, aq_send, e_send):
    rows, feat = x_hbm.shape
    part = rows // PARTS
    groups = rows // LANES
    scale = 0.5 * math.log2(math.e) / feat
    z = lax.axis_index('col')
    seg = lax.axis_index('seg')
    y, c = seg // 2, seg % 2
    corner = (z == 0) | (z == 3)
    near = 1 + z % 2
    far = 3 * (1 - z // 2)
    other = 6 - z - near - far
    plane = (1 - 2 * c) * 4 * PARTS

    def line(e):
        return jnp.where(e == 0, near, jnp.where(e == 1, other, far))

    def chunk(yy, zz, k):
        return ((2 * yy + c) * 4 + zz) * PARTS + k

    def block_of(ch):
        return ch // PARTS

    own = chunk(y, z, 0)
    DOWN, UP, SIDE, TWIN = range(4)
    device = [{'col': z - 1}, {'col': z + 1}, {'seg': 2 * (1 - y) + c}, {'seg': 2 * y + 1 - c}]

    def send(way, ch):
        pltpu.make_async_remote_copy(
            src_ref=xs.at[ch], dst_ref=xs.at[ch], send_sem=send_sem.at[way], recv_sem=recv_sem.at[ch],
            device_id=device[way], device_id_type=MESH).start()

    def send_if(cond, way, ch):
        @pl.when(cond)
        def _():
            send(way, ch)

    def arrive(ch):
        pltpu.make_async_copy(xs.at[ch], xs.at[ch], recv_sem.at[ch]).wait()

    def onward(zb, ch):
        send_if((zb > z) & (z > 0), DOWN, ch)
        send_if((zb < z) & (z < 3), UP, ch)

    def line_event(zb, k):
        ch = chunk(y, zb, k)
        arrive(ch)
        onward(zb, ch)
        send_if((k < PARTS - 1) | (zb - z == 3) | (z - zb == 3), SIDE, ch)
        send(TWIN, ch)

    def aq_copy(blk, dev, sem):
        return pltpu.make_async_remote_copy(
            src_ref=aq.at[blk], dst_ref=aq.at[blk], send_sem=sem, recv_sem=aq_recv.at[blk],
            device_id=dev, device_id_type=MESH)

    def aq_arrive(blk):
        pltpu.make_async_copy(aq.at[blk], aq.at[blk], aq_recv.at[blk]).wait()

    def aq_event(yy, zz):
        blk = block_of(chunk(yy, zz, 0))
        aq_arrive(blk)
        aq_copy(blk, device[TWIN], aq_send.at[1]).start()
        aq_arrive(blk + plane // PARTS)

    loads = [pltpu.make_async_copy(x_hbm.at[pl.ds(k * part, part)], xs.at[own + k], load_sem.at[k])
             for k in range(PARTS)]
    for load in loads:
        load.start()
    barrier = pltpu.get_barrier_semaphore()
    place = seg * 4 + z
    for d in range(1, 16):
        peer = (place + d) % 16
        pl.semaphore_signal(barrier, inc=1, device_id={'seg': peer // 4, 'col': peer % 4}, device_id_type=MESH)
    pl.semaphore_wait(barrier, 15)

    def send_own(k):
        send_if(z > 0, DOWN, own + k)
        send_if(z < 3, UP, own + k)
        send(SIDE, own + k)
        send(TWIN, own + k)

    for k in range(PARTS):
        loads[k].wait()
        if k < 2:
            send_own(k)

    for k in range(PARTS):
        wide = xs[own + k].astype(jnp.float32)
        a_col[pl.ds(k * part, part), :] = jnp.broadcast_to(
            scale * jnp.sum(wide * wide, axis=1, keepdims=True), (part, LANES))
    own_blk = block_of(own)
    for g in range(groups):
        span = pl.ds(g * LANES, LANES)
        aq[own_blk, g:g + 1, :] = jnp.transpose(a_col[span, :])[0:1, :]
        aq[own_blk, groups + g:groups + g + 1, :] = q_ref[g:g + 1, :]
        q_col[span, :] = jnp.transpose(jnp.broadcast_to(q_ref[g:g + 1, :], (LANES, LANES)))
    force[...] = jnp.zeros_like(force)
    row_sum[...] = jnp.zeros_like(row_sum)
    aq_copy(own_blk, device[TWIN], aq_send.at[1]).start()
    for d in range(1, 8):
        peer = (y * 4 + z + d) % 8
        aq_copy(own_blk, {'seg': 2 * (peer // 4) + c, 'col': peer % 4}, aq_send.at[0]).start()
    for k in range(2, PARTS):
        send_own(k)

    def tile(r, chunks, parts_of, masked):
        span = pl.ds(r * part, part)
        acc = force[span, :]
        total = row_sum[span, :]
        a_i = jnp.concatenate([a_col[span, :]] * 2, axis=1)
        q_i = jnp.concatenate([q_col[span, :]] * 2, axis=1)
        x_i = xs[own + r]
        for n, (ch, k) in enumerate(zip(chunks, parts_of)):
            x_j = xs[ch]
            blk = block_of(ch)
            def lanes(first):
                return jnp.concatenate([aq[blk, pl.ds(first + h, 1), :] for h in range(2)], axis=1)
            dots = lax.dot_general(x_i, x_j, NT, preferred_element_type=jnp.float32)
            power = jnp.minimum((2.0 * scale * dots - lanes(2 * k)) - a_i, 0.0)
            weights = (q_i * lanes(groups + 2 * k)) * jnp.exp2(power)
            if masked and n == r:
                rid = lax.broadcasted_iota(jnp.int32, weights.shape, 0)
                cid = lax.broadcasted_iota(jnp.int32, weights.shape, 1)
                weights = jnp.where(rid == cid, 0.0, weights)
            total = total + (weights[:, :LANES] + weights[:, LANES:])
            acc = acc + jnp.dot(weights.astype(jnp.bfloat16), x_j, preferred_element_type=jnp.float32)
        force[span, :] = acc
        row_sum[span, :] = total

    def pairs(chunks, parts_of, masked=False):
        for r in range(PARTS):
            tile(r, chunks, parts_of, masked)

    pairs([own + k for k in range(PARTS)], range(PARTS), masked=True)
    aq_arrive(own_blk + plane // PARTS)
    for k in range(PARTS):
        arrive(own + plane + k)
    pairs([own + plane + k for k in range(PARTS)], range(PARTS))

    LAST = PARTS - 1

    def step(u, carry):
        k4 = u % 4
        @pl.when(corner & (u < 12))
        def _():
            line_event(line(u // 4), k4)

        @pl.when(corner & (u >= 12))
        def _():
            ch = chunk(1 - y, line(u - 12), LAST)
            arrive(ch)
            send(TWIN, ch)

        @pl.when(~corner & (u < 4))
        def _():
            line_event(near, k4)
            line_event(other, k4)

        @pl.when(~corner & (u >= 4) & (u < 8))
        def _():
            line_event(far, k4)

        @pl.when(~corner & (u == 7))
        def _():
            ch = chunk(1 - y, z, LAST)
            send_if(z == 1, DOWN, ch)
            send_if(z == 2, UP, ch)

        @pl.when(~corner & (u >= 8) & (u < 11))
        def _():
            zb = line(u - 8)
            ch = chunk(1 - y, zb, LAST)
            arrive(ch)
            @pl.when(u < 10)
            def _():
                onward(zb, ch)
            send(TWIN, ch)

        side_zb = jnp.where(u < 4, z, jnp.where(u < 13, line((u - 4 + 3 * 4) // 3 - 4), far))
        side_k = jnp.where(u < 4, u, jnp.where(u < 13, (u - 4 + 3 * 4) % 3, LAST))
        side = chunk(1 - y, side_zb, side_k)

        @pl.when(corner | (u < 13))
        def _():
            arrive(side)
            send(TWIN, side)

        @pl.when(u == 3)
        def _():
            send_if(z < 2, UP, side)
            send_if(z >= 2, DOWN, side)

        for when, events in ((0, ((y, near), (1 - y, z))), (4, ((y, other), (1 - y, near))),
                             (7, ((1 - y, other),)), (8, ((y, far),)), (10, ((1 - y, far),))):
            @pl.when(u == when)
            def _():
                for yy, zz in events:
                    aq_event(yy, zz)

        along_y = jnp.where(u < 12, y, 1 - y)
        along_z = jnp.where(u < 12, line(u // 4), line(u - 12))
        along_k = jnp.where(u < 12, k4, LAST)
        along = chunk(along_y, along_z, along_k)
        arrive(along + plane)
        arrive(side + plane)
        pairs([along, side, along + plane, side + plane], [along_k, side_k, along_k, side_k])
        return carry

    lax.fori_loop(0, 14, step, 0)

    tile_sum = jnp.sum(row_sum[...].reshape(rows // 8, 8, LANES), axis=0)
    es[place] = tile_sum
    def e_copy(peer):
        return pltpu.make_async_remote_copy(
            src_ref=es.at[place], dst_ref=es.at[place], send_sem=e_send, recv_sem=e_recv,
            device_id={'seg': peer // 4, 'col': peer % 4}, device_id_type=MESH)
    for d in range(1, 16):
        e_copy((place + d) % 16).start()

    inv_len2 = 1.0 / feat
    for r in range(PARTS):
        span = pl.ds(r * part, part)
        full = jnp.sum(row_sum[span, :], axis=1, keepdims=True)
        out_ref[span, :] = (full * xs[own + r].astype(jnp.float32) - force[span, :]) * inv_len2

    def drain(sem, ref):
        pltpu.make_async_copy(ref, ref, sem).wait()

    drain(send_sem.at[TWIN], xs.at[pl.ds(0, 8 * PARTS)])
    drain(aq_send.at[0], aq.at[pl.ds(0, 7)])
    drain(aq_send.at[1], aq.at[pl.ds(0, 8)])
    for zz, counts in enumerate(((0, 5, 14), (14, 10, 13), (10, 14, 13), (5, 0, 14))):
        @pl.when(z == zz)
        def _():
            for way, count in zip((DOWN, UP, SIDE), counts):
                if count:
                    drain(send_sem.at[way], xs.at[pl.ds(0, count)])
    drain(e_recv, es.at[pl.ds(0, 15)])
    drain(e_send, es.at[pl.ds(0, 15)])
    e_ref[0] = 0.5 * jnp.sum(es[...])


def solution(mesh):
    assert (mesh.shape['seg'], mesh.shape['col']) == (4, 4)

    def per_device(x_own, q_own):
        rows, feat = x_own.shape
        part = rows // PARTS
        groups = rows // LANES
        f32, bf16 = jnp.float32, jnp.bfloat16
        vmem = pltpu.VMEM
        dma = pltpu.SemaphoreType.DMA
        return pl.pallas_call(
            pair_kernel,
            out_shape=(jax.ShapeDtypeStruct((rows, feat), f32), jax.ShapeDtypeStruct((1,), f32)),
            in_specs=[pl.BlockSpec(memory_space=pl.ANY), pl.BlockSpec(memory_space=vmem)],
            out_specs=(pl.BlockSpec(memory_space=vmem), pl.BlockSpec(memory_space=pltpu.SMEM)),
            scratch_shapes=[
                vmem((16 * PARTS, part, feat), bf16), vmem((16, 2 * groups, LANES), f32), vmem((16, 8, LANES), f32),
                vmem((rows, LANES), f32), vmem((rows, LANES), f32), vmem((rows, feat), f32), vmem((rows, LANES), f32),
                dma((PARTS,)), dma((16 * PARTS,)), dma((16,)), dma, dma((4,)), dma((2,)), dma],
            compiler_params=pltpu.CompilerParams(
                collective_id=0, has_side_effects=True, vmem_limit_bytes=40 * 2 ** 20),
        )(x_own, q_own.reshape(groups, LANES))

    row_spec = P(ROW_AXES, None)
    return jax.shard_map(per_device, mesh=mesh, in_specs=(row_spec, P(ROW_AXES)),
                         out_specs=(row_spec, P('sys')), check_vma=False)
```

```python
import functools
import math

import jax
import jax.numpy as jnp
from jax import lax
from jax.experimental import pallas as pl
from jax.experimental.pallas import tpu as pltpu
from jax.sharding import PartitionSpec as P

ROW_AXES = ('sys', 'seg', 'col')
MESH = pl.DeviceIdType.MESH
NT = (((1,), (1,)), ((), ()))
PARTS = 4
LANES = 128


def pair_kernel(x_hbm, q_hbm, out_ref, e_ref, xs, aq, es, q_ref, a_col, q_col, force, row_sum,
                load_sem, recv_sem, aq_recv, e_recv, send_sem, aq_send, e_send):
    rows, feat = x_hbm.shape
    part = rows // PARTS
    groups = rows // LANES
    scale = 0.5 * math.log2(math.e) / feat
    z = lax.axis_index('col')
    seg = lax.axis_index('seg')
    y, c = seg // 2, seg % 2
    corner = (z == 0) | (z == 3)
    near = 1 + z % 2
    far = 3 * (1 - z // 2)
    other = 6 - z - near - far
    plane = (1 - 2 * c) * 4 * PARTS

    def line(e):
        return jnp.where(e == 0, near, jnp.where(e == 1, other, far))

    def chunk(yy, zz, k):
        return ((2 * yy + c) * 4 + zz) * PARTS + k

    def block_of(ch):
        return ch // PARTS

    own = chunk(y, z, 0)
    DOWN, UP, SIDE, TWIN = range(4)
    device = [{'col': z - 1}, {'col': z + 1}, {'seg': 2 * (1 - y) + c}, {'seg': 2 * y + 1 - c}]

    def send(way, ch):
        pltpu.make_async_remote_copy(
            src_ref=xs.at[ch], dst_ref=xs.at[ch], send_sem=send_sem.at[way], recv_sem=recv_sem.at[ch],
            device_id=device[way], device_id_type=MESH).start()

    def send_if(cond, way, ch):
        @pl.when(cond)
        def _():
            send(way, ch)

    def arrive(ch):
        pltpu.make_async_copy(xs.at[ch], xs.at[ch], recv_sem.at[ch]).wait()

    def onward(zb, ch):
        send_if((zb > z) & (z > 0), DOWN, ch)
        send_if((zb < z) & (z < 3), UP, ch)

    def aq_send_to(way, blk):
        pltpu.make_async_remote_copy(
            src_ref=aq.at[blk], dst_ref=aq.at[blk], send_sem=aq_send.at[way], recv_sem=aq_recv.at[blk],
            device_id=device[way], device_id_type=MESH).start()

    def aq_send_if(cond, way, blk):
        @pl.when(cond)
        def _():
            aq_send_to(way, blk)

    def aq_arrive(blk):
        pltpu.make_async_copy(aq.at[blk], aq.at[blk], aq_recv.at[blk]).wait()

    def line_event(zb, k):
        ch = chunk(y, zb, k)
        arrive(ch)
        onward(zb, ch)
        send_if((k < PARTS - 1) | (zb - z == 3) | (z - zb == 3), SIDE, ch)
        send(TWIN, ch)

        @pl.when(k == 0)
        def _():
            blk = block_of(ch)
            aq_arrive(blk)
            aq_send_if((zb > z) & (z > 0), DOWN, blk)
            aq_send_if((zb < z) & (z < 3), UP, blk)
            aq_send_to(SIDE, blk)
            aq_send_to(TWIN, blk)

    loads = [pltpu.make_async_copy(x_hbm.at[pl.ds(k * part, part)], xs.at[own + k], load_sem.at[k])
             for k in range(PARTS)]
    loads.append(pltpu.make_async_copy(q_hbm, q_ref, load_sem.at[PARTS]))
    for load in loads:
        load.start()
    barrier = pltpu.get_barrier_semaphore()

    def greet(way):
        pl.semaphore_signal(barrier, inc=1, device_id=device[way], device_id_type=MESH)

    pl.when(z > 0)(lambda: greet(DOWN))
    pl.when(z < 3)(lambda: greet(UP))
    greet(SIDE)
    greet(TWIN)

    own_blk = block_of(own)
    loads[PARTS].wait()
    for k in range(PARTS):
        loads[k].wait()
        wide = xs[own + k].astype(jnp.float32)
        a_col[pl.ds(k * part, part), :] = jnp.broadcast_to(
            scale * jnp.sum(wide * wide, axis=1, keepdims=True), (part, LANES))
    for g in range(groups):
        span = pl.ds(g * LANES, LANES)
        aq[own_blk, g:g + 1, :] = jnp.transpose(a_col[span, :])[0:1, :]
        aq[own_blk, groups + g:groups + g + 1, :] = q_ref[g:g + 1, :]
        q_col[span, :] = jnp.transpose(jnp.broadcast_to(q_ref[g:g + 1, :], (LANES, LANES)))

    pl.semaphore_wait(barrier, jnp.where(corner, 3, 4))
    for k in range(PARTS):
        send_if(z > 0, DOWN, own + k)
        send_if(z < 3, UP, own + k)
        send(SIDE, own + k)
        send(TWIN, own + k)
        if k == 0:
            aq_send_if(z > 0, DOWN, own_blk)
            aq_send_if(z < 3, UP, own_blk)
            aq_send_to(SIDE, own_blk)
            aq_send_to(TWIN, own_blk)
    force[...] = jnp.zeros_like(force)
    row_sum[...] = jnp.zeros_like(row_sum)

    def tile(r, chunks, parts_of, masked):
        span = pl.ds(r * part, part)
        acc = force[span, :]
        total = row_sum[span, :]
        a_i = jnp.concatenate([a_col[span, :]] * 2, axis=1)
        q_i = jnp.concatenate([q_col[span, :]] * 2, axis=1)
        x_i = xs[own + r]
        for n, (ch, k) in enumerate(zip(chunks, parts_of)):
            x_j = xs[ch]
            blk = block_of(ch)
            def lanes(first):
                return jnp.concatenate([aq[blk, pl.ds(first + h, 1), :] for h in range(2)], axis=1)
            dots = lax.dot_general(x_i, x_j, NT, preferred_element_type=jnp.float32)
            power = jnp.minimum((2.0 * scale * dots - lanes(2 * k)) - a_i, 0.0)
            weights = (q_i * lanes(groups + 2 * k)) * jnp.exp2(power)
            if masked and n == r:
                rid = lax.broadcasted_iota(jnp.int32, weights.shape, 0)
                cid = lax.broadcasted_iota(jnp.int32, weights.shape, 1)
                weights = jnp.where(rid == cid, 0.0, weights)
            total = total + (weights[:, :LANES] + weights[:, LANES:])
            acc = acc + jnp.dot(weights.astype(jnp.bfloat16), x_j, preferred_element_type=jnp.float32)
        force[span, :] = acc
        row_sum[span, :] = total

    def pairs(chunks, parts_of, masked=False):
        for r in range(PARTS):
            tile(r, chunks, parts_of, masked)

    pairs([own + k for k in range(PARTS)], range(PARTS), masked=True)
    aq_arrive(own_blk + plane // PARTS)
    for k in range(PARTS):
        arrive(own + plane + k)
    pairs([own + plane + k for k in range(2)], range(2))

    LAST = PARTS - 1

    def step(u, carry):
        k4 = u % 4
        @pl.when(corner & (u < 12))
        def _():
            line_event(line(u // 4), k4)

        @pl.when(corner & (u >= 12))
        def _():
            ch = chunk(1 - y, line(u - 12), LAST)
            arrive(ch)
            send(TWIN, ch)

        @pl.when(~corner & (u < 4))
        def _():
            line_event(near, k4)
            line_event(other, k4)

        @pl.when(~corner & (u >= 4) & (u < 8))
        def _():
            line_event(far, k4)

        @pl.when(~corner & (u == 7))
        def _():
            ch = chunk(1 - y, z, LAST)
            send_if(z == 1, DOWN, ch)
            send_if(z == 2, UP, ch)

        @pl.when(~corner & (u >= 8) & (u < 11))
        def _():
            zb = line(u - 8)
            ch = chunk(1 - y, zb, LAST)
            arrive(ch)
            @pl.when(u < 10)
            def _():
                onward(zb, ch)
            send(TWIN, ch)

        side_zb = jnp.where(u < 4, z, jnp.where(u < 13, line((u - 4 + 3 * 4) // 3 - 4), far))
        side_k = jnp.where(u < 4, u, jnp.where(u < 13, (u - 4 + 3 * 4) % 3, LAST))
        side = chunk(1 - y, side_zb, side_k)

        @pl.when(corner | (u < 13))
        def _():
            arrive(side)
            send(TWIN, side)

        @pl.when(u == 3)
        def _():
            send_if(z < 2, UP, side)
            send_if(z >= 2, DOWN, side)

        @pl.when((u == 0) | (u == 4) | (u == 7) | (u == 10))
        def _():
            blk = block_of(side)
            aq_arrive(blk)
            aq_send_to(TWIN, blk)

        along = jnp.where(u < 12, chunk(y, line(u // 4), k4), chunk(1 - y, line(u - 12), LAST))
        pairs_of_step(u, along, side, carry)
        return along, side

    def from_twin(u, along, side):
        @pl.when((u == 0) | (u == 4) | (u == 8))
        def _():
            aq_arrive(block_of(along))

        @pl.when((u == 0) | (u == 4) | (u == 7) | (u == 10))
        def _():
            aq_arrive(block_of(side))

        arrive(along)
        arrive(side)

    def pairs_of_step(u, along, side, before):
        along_before, side_before = (ch + plane for ch in before)

        @pl.when(u > 0)
        def _():
            from_twin(u - 1, along_before, side_before)

        chunks = [along, side, along_before, side_before]
        pairs(chunks, [ch % PARTS for ch in chunks])

    along, side = lax.fori_loop(0, 14, step, (own + 2, own + 3))
    from_twin(13, along + plane, side + plane)
    pairs([along + plane, side + plane], [along % PARTS, side % PARTS])

    place = seg * 4 + z
    tile_sum = jnp.sum(row_sum[...].reshape(rows // 8, 8, LANES), axis=0)
    es[place] = tile_sum
    def e_copy(peer):
        return pltpu.make_async_remote_copy(
            src_ref=es.at[place], dst_ref=es.at[place], send_sem=e_send, recv_sem=e_recv,
            device_id={'seg': peer // 4, 'col': peer % 4}, device_id_type=MESH)
    for d in range(1, 16):
        e_copy((place + d) % 16).start()

    inv_len2 = 1.0 / feat
    for r in range(PARTS):
        span = pl.ds(r * part, part)
        full = jnp.sum(row_sum[span, :], axis=1, keepdims=True)
        out_ref[span, :] = (full * xs[own + r].astype(jnp.float32) - force[span, :]) * inv_len2

    def drain(sem, ref):
        pltpu.make_async_copy(ref, ref, sem).wait()

    drain(send_sem.at[TWIN], xs.at[pl.ds(0, 8 * PARTS)])
    drain(aq_send.at[TWIN], aq.at[pl.ds(0, 8)])
    drain(aq_send.at[SIDE], aq.at[pl.ds(0, 4)])
    for zz, counts in enumerate(((0, 5, 14), (14, 10, 13), (10, 14, 13), (5, 0, 14))):
        @pl.when(z == zz)
        def _():
            for way, count in zip((DOWN, UP, SIDE), counts):
                if count:
                    drain(send_sem.at[way], xs.at[pl.ds(0, count)])
            if zz:
                drain(aq_send.at[DOWN], aq.at[pl.ds(0, 4 - zz)])
            if zz < 3:
                drain(aq_send.at[UP], aq.at[pl.ds(0, zz + 1)])
    drain(e_recv, es.at[pl.ds(0, 15)])
    drain(e_send, es.at[pl.ds(0, 15)])
    e_ref[0] = 0.5 * jnp.sum(es[...])


def solution(mesh):
    assert (mesh.shape['seg'], mesh.shape['col']) == (4, 4)

    def per_device(x_own, q_own):
        rows, feat = x_own.shape
        part = rows // PARTS
        groups = rows // LANES
        f32, bf16 = jnp.float32, jnp.bfloat16
        vmem = pltpu.VMEM
        dma = pltpu.SemaphoreType.DMA
        return pl.pallas_call(
            pair_kernel,
            out_shape=(jax.ShapeDtypeStruct((rows, feat), f32), jax.ShapeDtypeStruct((1,), f32)),
            in_specs=[pl.BlockSpec(memory_space=pltpu.HBM)] * 2,
            out_specs=(pl.BlockSpec(memory_space=vmem), pl.BlockSpec(memory_space=pltpu.SMEM)),
            scratch_shapes=[
                vmem((16 * PARTS, part, feat), bf16), vmem((16, 2 * groups, LANES), f32), vmem((16, 8, LANES), f32),
                vmem((groups, LANES), f32),
                vmem((rows, LANES), f32), vmem((rows, LANES), f32), vmem((rows, feat), f32), vmem((rows, LANES), f32),
                dma((PARTS + 1,)), dma((16 * PARTS,)), dma((16,)), dma, dma((4,)), dma((4,)), dma],
            compiler_params=pltpu.CompilerParams(
                collective_id=0, has_side_effects=True, vmem_limit_bytes=40 * 2 ** 20),
        )(x_own, q_own.reshape(groups, LANES))

    row_spec = P(ROW_AXES, None)
    return jax.shard_map(per_device, mesh=mesh, in_specs=(row_spec, P(ROW_AXES)),
                         out_specs=(row_spec, P('sys')), check_vma=False)
```

```python
import functools
import math

import jax
import jax.numpy as jnp
from jax import lax
from jax.experimental import pallas as pl
from jax.experimental.pallas import tpu as pltpu
from jax.sharding import PartitionSpec as P

ROW_AXES = ('sys', 'seg', 'col')
MESH = pl.DeviceIdType.MESH
NT = (((1,), (1,)), ((), ()))
PARTS = 4
LANES = 128


def pair_kernel(x_hbm, q_hbm, out_ref, e_ref, xs, aq, es, e_acc, q_ref, a_col, q_col,
                a_end, q_end, force, row_sum,
                load_sem, recv_sem, aq_recv, e_recv, send_sem, aq_send, e_send):
    rows, feat = x_hbm.shape
    part = rows // PARTS
    groups = rows // LANES
    scale = 0.5 * math.log2(math.e) / feat
    z = lax.axis_index('col')
    seg = lax.axis_index('seg')
    y, c = seg // 2, seg % 2
    corner = (z == 0) | (z == 3)
    near = 1 + z % 2
    far = 3 * (1 - z // 2)
    other = 6 - z - near - far
    plane = (1 - 2 * c) * 4 * PARTS

    def line(e):
        return jnp.where(e == 0, near, jnp.where(e == 1, other, far))

    def chunk(yy, zz, k):
        return ((2 * yy + c) * 4 + zz) * PARTS + k

    def block_of(ch):
        return ch // PARTS

    own = chunk(y, z, 0)
    LAST = PARTS - 1
    DOWN, UP, SIDE, TWIN = range(4)
    device = [{'col': z - 1}, {'col': z + 1}, {'seg': 2 * (1 - y) + c}, {'seg': 2 * y + 1 - c}]

    def send(way, ch):
        pltpu.make_async_remote_copy(
            src_ref=xs.at[ch], dst_ref=xs.at[ch], send_sem=send_sem.at[way], recv_sem=recv_sem.at[ch],
            device_id=device[way], device_id_type=MESH).start()

    def send_if(cond, way, ch):
        @pl.when(cond)
        def _():
            send(way, ch)

    def arrive(ch):
        pltpu.make_async_copy(xs.at[ch], xs.at[ch], recv_sem.at[ch]).wait()

    def onward(zb, ch):
        send_if((zb > z) & (z > 0), DOWN, ch)
        send_if((zb < z) & (z < 3), UP, ch)

    def aq_send_to(way, blk):
        pltpu.make_async_remote_copy(
            src_ref=aq.at[blk], dst_ref=aq.at[blk], send_sem=aq_send.at[way], recv_sem=aq_recv.at[blk],
            device_id=device[way], device_id_type=MESH).start()

    def aq_send_if(cond, way, blk):
        @pl.when(cond)
        def _():
            aq_send_to(way, blk)

    def aq_arrive(blk):
        pltpu.make_async_copy(aq.at[blk], aq.at[blk], aq_recv.at[blk]).wait()

    def line_event(zb, k):
        ch = chunk(y, zb, k)
        arrive(ch)
        onward(zb, ch)
        near_side = jnp.where((zb == near) | (corner & (zb == other)), 3, 2)
        send_if(k < jnp.where(corner & (zb == far), PARTS, near_side), SIDE, ch)
        send(TWIN, ch)

        @pl.when(k == 0)
        def _():
            blk = block_of(ch)
            aq_arrive(blk)
            aq_send_if((zb > z) & (z > 0), DOWN, blk)
            aq_send_if((zb < z) & (z < 3), UP, blk)
            aq_send_to(SIDE, blk)
            aq_send_to(TWIN, blk)

    loads = [pltpu.make_async_copy(x_hbm.at[pl.ds(k * part, part)], xs.at[own + k], load_sem.at[k])
             for k in range(PARTS)]
    loads.append(pltpu.make_async_copy(q_hbm, q_ref, load_sem.at[PARTS]))
    for load in loads:
        load.start()
    barrier = pltpu.get_barrier_semaphore()

    def greet(way):
        pl.semaphore_signal(barrier, inc=1, device_id=device[way], device_id_type=MESH)

    pl.when(z > 0)(lambda: greet(DOWN))
    pl.when(z < 3)(lambda: greet(UP))
    greet(SIDE)
    greet(TWIN)

    own_blk = block_of(own)
    loads[PARTS].wait()
    for k in range(PARTS):
        loads[k].wait()
        wide = xs[own + k].astype(jnp.float32)
        a_col[pl.ds(k * part, part), :] = jnp.broadcast_to(
            scale * jnp.sum(wide * wide, axis=1, keepdims=True), (part, LANES))
    for g in range(groups):
        span = pl.ds(g * LANES, LANES)
        aq[own_blk, g:g + 1, :] = jnp.transpose(a_col[span, :])[0:1, :]
        aq[own_blk, groups + g:groups + g + 1, :] = q_ref[g:g + 1, :]
        q_col[span, :] = jnp.transpose(jnp.broadcast_to(q_ref[g:g + 1, :], (LANES, LANES)))

    pl.semaphore_wait(barrier, jnp.where(corner, 3, 4))
    for k in range(PARTS):
        send_if(z > 0, DOWN, own + k)
        send_if(z < 3, UP, own + k)
        send(SIDE, own + k)
        send(TWIN, own + k)
        if k == 0:
            aq_send_if(z > 0, DOWN, own_blk)
            aq_send_if(z < 3, UP, own_blk)
            aq_send_to(SIDE, own_blk)
            aq_send_to(TWIN, own_blk)
    force[...] = jnp.zeros_like(force)
    row_sum[...] = jnp.zeros_like(row_sum)
    e_acc[...] = jnp.zeros_like(e_acc)

    def share(ch):
        same_line = (block_of(ch) // 8) == y
        z_j = block_of(ch) % 4
        at_corner = jnp.where((z_j == z) | ((z_j == far) & same_line), 0.5, 0.0)
        at_middle = jnp.where((z_j == 1) | (z_j == 2), 0.5, 1.0)
        return jnp.where(corner, at_corner, at_middle)

    def weights_of(x_i, a_i, q_i, ch, k):
        blk = block_of(ch)
        def lanes(first):
            return jnp.concatenate([aq[blk, pl.ds(first + h, 1), :] for h in range(2)], axis=1)
        a_i, q_i = (jnp.concatenate([v] * 2, axis=1) for v in (a_i, q_i))
        dots = lax.dot_general(x_i, xs[ch], NT, preferred_element_type=jnp.float32)
        power = jnp.minimum((2.0 * scale * dots - lanes(2 * k)) - a_i, 0.0)
        return (q_i * lanes(groups + 2 * k)) * jnp.exp2(power)

    def fold(weights):
        return weights[:, :LANES] + weights[:, LANES:]

    def stack(halves):
        return jnp.sum(halves.reshape(part // 8, 8, LANES), axis=0)

    def tile(r, chunks, parts_of, masked):
        span = pl.ds(r * part, part)
        acc = force[span, :]
        total = row_sum[span, :]
        e_part = jnp.zeros((8, LANES), jnp.float32)
        for n, (ch, k) in enumerate(zip(chunks, parts_of)):
            weights = weights_of(xs[own + r], a_col[span, :], q_col[span, :], ch, k)
            if masked and n == r:
                rid = lax.broadcasted_iota(jnp.int32, weights.shape, 0)
                cid = lax.broadcasted_iota(jnp.int32, weights.shape, 1)
                weights = jnp.where(rid == cid, 0.0, weights)
            halves = fold(weights)
            total = total + halves
            e_part = e_part + share(ch) * stack(halves)
            acc = acc + jnp.dot(weights.astype(jnp.bfloat16), xs[ch], preferred_element_type=jnp.float32)
        force[span, :] = acc
        row_sum[span, :] = total
        e_acc[...] += e_part

    def pairs(chunks, parts_of, masked=False):
        for r in range(PARTS):
            tile(r, chunks, parts_of, masked)

    end_rows = chunk(y, 0, 0)
    end_cols = ((2 * (1 - y) + z - 1) * 4 + 3) * PARTS

    def end_vectors():
        blk = block_of(end_rows)
        for g in range(groups):
            for ref, first in ((a_end, 0), (q_end, groups)):
                row = aq[blk, first + g:first + g + 1, :]
                ref[pl.ds(g * LANES, LANES), :] = jnp.transpose(jnp.broadcast_to(row, (LANES, LANES)))

    def end_energy(k):
        e_part = jnp.zeros((8, LANES), jnp.float32)
        for r in range(PARTS):
            span = pl.ds(r * part, part)
            e_part = e_part + stack(fold(weights_of(
                xs[end_rows + r], a_end[span, :], q_end[span, :], end_cols + k, k)))
        e_acc[...] += e_part

    pairs([own + k for k in range(PARTS)], range(PARTS), masked=True)
    aq_arrive(own_blk + plane // PARTS)
    for k in range(PARTS):
        arrive(own + plane + k)
    pairs([own + plane + k for k in range(2)], range(2))

    place = seg * 4 + z

    def send_energy():
        for d in range(1, 16):
            peer = (place + d) % 16
            pltpu.make_async_remote_copy(
                src_ref=es.at[place], dst_ref=es.at[place], send_sem=e_send, recv_sem=e_recv,
                device_id={'seg': peer // 4, 'col': peer % 4}, device_id_type=MESH).start()

    def cross_event(zb, k, pass_on):
        ch = chunk(1 - y, zb, k)
        arrive(ch)
        if pass_on:
            onward(zb, ch)
        send(TWIN, ch)

    def schedule(u):
        k4 = u % 4
        v = u + 8
        along_corner = jnp.where(u < 12, chunk(y, line(u // 4), k4), chunk(1 - y, line(u - 12), LAST))
        along_middle = jnp.where(u < 8, chunk(y, jnp.where(u < 4, near, far), k4),
                                 jnp.where(u == 8, chunk(1 - y, near, 2), chunk(1 - y, far, u - 9)))
        side_corner = chunk(1 - y, jnp.where(u < 13, line(v // 3 - 4), far), jnp.where(u < 13, v % 3, LAST))
        side_middle = jnp.where(
            u < 8, chunk(1 - y, jnp.where(u % 2 == 0, near, other), v // 2 - 6),
            jnp.where(u < 10, chunk(1 - y, other, u - 6), chunk(1 - y, jnp.where(u == 10, near, far), LAST)))
        side = jnp.where(u < 4, chunk(1 - y, z, u), jnp.where(corner, side_corner, side_middle))
        return jnp.where(corner, along_corner, along_middle), side

    def cross_opens(u):
        return (u == 0) | (u == 4) | (corner & ((u == 7) | (u == 10))) | (~corner & ((u == 5) | (u == 9)))

    def evaluate(chunks):
        pairs(chunks, [ch % PARTS for ch in chunks])

    def from_twin(u):
        along, side = (ch + plane for ch in schedule(u))

        @pl.when((u == 0) | (u == 4) | (corner & (u == 8)))
        def _():
            aq_arrive(block_of(along))

        @pl.when(cross_opens(u))
        def _():
            aq_arrive(block_of(jnp.where(~corner & (u == 9), along, side)))

        arrive(along)
        arrive(side)
        evaluate([along, side])

    def step(u, carry):
        @pl.when(u == 0)
        def _():
            evaluate([own + plane + 2, own + plane + 3])

        @pl.when((u > 0) & (corner | (u < 13)))
        def _():
            from_twin(u - 1)

        @pl.when(corner & (u == 12))
        def _():
            es[place] = e_acc[...]

        along, side = schedule(u)

        @pl.when(corner & (u < 12))
        def _():
            line_event(line(u // 4), u % 4)

        @pl.when(corner & (u >= 12))
        def _():
            cross_event(line(u - 12), LAST, False)

        @pl.when(~corner & (u < 4))
        def _():
            line_event(near, u)
            line_event(other, u)

        @pl.when(~corner & (u >= 4) & (u < 8))
        def _():
            line_event(far, u - 4)

        @pl.when(~corner & (u == 7))
        def _():
            ch = chunk(1 - y, z, LAST)
            send_if(z == 1, DOWN, ch)
            send_if(z == 2, UP, ch)

        @pl.when(~corner & ((u == 6) | (u == 7)))
        def _():
            cross_event(other, u - 4, True)

        @pl.when(~corner & (u == 9))
        def _():
            cross_event(near, LAST, True)

        @pl.when(~corner & (u == 11))
        def _():
            cross_event(far, 2, False)
            cross_event(far, LAST, False)

        @pl.when(corner | (u < 11))
        def _():
            ch = jnp.where(~corner & (u >= 8), along, side)
            arrive(ch)
            send(TWIN, ch)

        @pl.when((u == 3) | (corner & (u == 2)))
        def _():
            send_if(z < 2, UP, side)
            send_if(z >= 2, DOWN, side)

        @pl.when(cross_opens(u))
        def _():
            blk = block_of(jnp.where(~corner & (u == 9), along, side))
            aq_arrive(blk)
            aq_send_to(TWIN, blk)

        pl.when(corner & (u == 12))(send_energy)

        @pl.when(corner | (u < 12))
        def _():
            evaluate([along, side])

        @pl.when(~corner & ((u == 1) | (u == 3)))
        def _():
            pair = [chunk(y, other, u - 1), chunk(y, other, u)]

            @pl.when(u == 1)
            def _():
                aq_arrive(block_of(pair[0] + plane))

            for ch in pair:
                arrive(ch + plane)
            evaluate(pair + [ch + plane for ch in pair])

        pl.when(~corner & (u == 8))(end_vectors)
        pl.when(~corner & (u >= 10))(lambda: end_energy(u - 10))
        return carry

    lax.fori_loop(0, 14, step, 0)
    pl.when(corner)(lambda: from_twin(13))

    @pl.when(~corner)
    def _():
        es[place] = e_acc[...]

    def drain(sem, ref):
        pltpu.make_async_copy(ref, ref, sem).wait()

    drain(send_sem.at[TWIN], xs.at[pl.ds(0, 8 * PARTS)])
    pl.when(~corner)(send_energy)

    inv_len2 = 1.0 / feat
    for r in range(PARTS):
        span = pl.ds(r * part, part)
        full = jnp.sum(row_sum[span, :], axis=1, keepdims=True)
        out_ref[span, :] = (full * xs[own + r].astype(jnp.float32) - force[span, :]) * inv_len2

    drain(aq_send.at[TWIN], aq.at[pl.ds(0, 8)])
    drain(aq_send.at[SIDE], aq.at[pl.ds(0, 4)])
    for zz, counts in enumerate(((0, 6, 14), (14, 11, 11), (11, 14, 11), (6, 0, 14))):
        @pl.when(z == zz)
        def _():
            for way, count in zip((DOWN, UP, SIDE), counts):
                if count:
                    drain(send_sem.at[way], xs.at[pl.ds(0, count)])
            if zz:
                drain(aq_send.at[DOWN], aq.at[pl.ds(0, 4 - zz)])
            if zz < 3:
                drain(aq_send.at[UP], aq.at[pl.ds(0, zz + 1)])
    drain(e_recv, es.at[pl.ds(0, 15)])
    drain(e_send, es.at[pl.ds(0, 15)])
    e_ref[0] = jnp.sum(es[...])


def solution(mesh):
    assert (mesh.shape['seg'], mesh.shape['col']) == (4, 4)

    def per_device(x_own, q_own):
        rows, feat = x_own.shape
        part = rows // PARTS
        groups = rows // LANES
        f32, bf16 = jnp.float32, jnp.bfloat16
        vmem = pltpu.VMEM
        dma = pltpu.SemaphoreType.DMA
        return pl.pallas_call(
            pair_kernel,
            out_shape=(jax.ShapeDtypeStruct((rows, feat), f32), jax.ShapeDtypeStruct((1,), f32)),
            in_specs=[pl.BlockSpec(memory_space=pltpu.HBM)] * 2,
            out_specs=(pl.BlockSpec(memory_space=vmem), pl.BlockSpec(memory_space=pltpu.SMEM)),
            scratch_shapes=[
                vmem((16 * PARTS, part, feat), bf16), vmem((16, 2 * groups, LANES), f32), vmem((16, 8, LANES), f32),
                vmem((8, LANES), f32), vmem((groups, LANES), f32),
                vmem((rows, LANES), f32), vmem((rows, LANES), f32), vmem((rows, LANES), f32), vmem((rows, LANES), f32),
                vmem((rows, feat), f32), vmem((rows, LANES), f32),
                dma((PARTS + 1,)), dma((16 * PARTS,)), dma((16,)), dma, dma((4,)), dma((4,)), dma],
            compiler_params=pltpu.CompilerParams(
                collective_id=0, has_side_effects=True, vmem_limit_bytes=40 * 2 ** 20),
        )(*(pltpu.with_memory_space_constraint(v, pltpu.HBM) for v in (x_own, q_own.reshape(groups, LANES))))

    row_spec = P(ROW_AXES, None)
    return jax.shard_map(per_device, mesh=mesh, in_specs=(row_spec, P(ROW_AXES)),
                         out_specs=(row_spec, P('sys')), check_vma=False)
```

```python
import functools
import math

import jax
import jax.numpy as jnp
from jax import lax
from jax.experimental import pallas as pl
from jax.experimental.pallas import tpu as pltpu
from jax.sharding import PartitionSpec as P

ROW_AXES = ('sys', 'seg', 'col')
MESH = pl.DeviceIdType.MESH
NT = (((1,), (1,)), ((), ()))
PARTS = 4
LANES = 128


def pair_kernel(x_hbm, q_hbm, out_ref, e_ref, xs, aq, es, e_acc, q_ref, a_col, q_col,
                a_end, q_end, force, row_sum,
                load_sem, recv_sem, aq_recv, e_recv, send_sem, aq_send, e_send):
    rows, feat = x_hbm.shape
    part = rows // PARTS
    groups = rows // LANES
    scale = 0.5 * math.log2(math.e) / feat
    z = lax.axis_index('col')
    seg = lax.axis_index('seg')
    y, c = seg // 2, seg % 2
    corner = (z == 0) | (z == 3)
    near = 1 + z % 2
    far = 3 * (1 - z // 2)
    other = 6 - z - near - far
    plane = (1 - 2 * c) * 4 * PARTS

    def line(e):
        return jnp.where(e == 0, near, jnp.where(e == 1, other, far))

    def chunk(yy, zz, k):
        return ((2 * yy + c) * 4 + zz) * PARTS + k

    def block_of(ch):
        return ch // PARTS

    own = chunk(y, z, 0)
    LAST = PARTS - 1
    DOWN, UP, SIDE, TWIN = range(4)
    device = [{'col': z - 1}, {'col': z + 1}, {'seg': 2 * (1 - y) + c}, {'seg': 2 * y + 1 - c}]

    def send(way, ch):
        pltpu.make_async_remote_copy(
            src_ref=xs.at[ch], dst_ref=xs.at[ch], send_sem=send_sem.at[way], recv_sem=recv_sem.at[ch],
            device_id=device[way], device_id_type=MESH).start()

    def send_if(cond, way, ch):
        @pl.when(cond)
        def _():
            send(way, ch)

    def arrive(ch):
        pltpu.make_async_copy(xs.at[ch], xs.at[ch], recv_sem.at[ch]).wait()

    def onward(zb, ch):
        send_if((zb > z) & (z > 0), DOWN, ch)
        send_if((zb < z) & (z < 3), UP, ch)

    def aq_send_to(way, blk):
        pltpu.make_async_remote_copy(
            src_ref=aq.at[blk], dst_ref=aq.at[blk], send_sem=aq_send.at[way], recv_sem=aq_recv.at[blk],
            device_id=device[way], device_id_type=MESH).start()

    def aq_send_if(cond, way, blk):
        @pl.when(cond)
        def _():
            aq_send_to(way, blk)

    def aq_arrive(blk):
        pltpu.make_async_copy(aq.at[blk], aq.at[blk], aq_recv.at[blk]).wait()

    def line_event(zb, k):
        ch = chunk(y, zb, k)
        arrive(ch)
        onward(zb, ch)
        near_side = jnp.where((zb == near) | (corner & (zb == other)), 3, 2)
        send_if(k < jnp.where(corner & (zb == far), PARTS, near_side), SIDE, ch)
        send(TWIN, ch)

        @pl.when(k == 0)
        def _():
            blk = block_of(ch)
            aq_arrive(blk)
            aq_send_if((zb > z) & (z > 0), DOWN, blk)
            aq_send_if((zb < z) & (z < 3), UP, blk)
            aq_send_to(SIDE, blk)
            aq_send_to(TWIN, blk)

    loads = [pltpu.make_async_copy(x_hbm.at[pl.ds(k * part, part)], xs.at[own + k], load_sem.at[k])
             for k in range(PARTS)]
    loads.append(pltpu.make_async_copy(q_hbm, q_ref, load_sem.at[PARTS]))
    for load in loads:
        load.start()
    barrier = pltpu.get_barrier_semaphore()

    def greet(way):
        pl.semaphore_signal(barrier, inc=1, device_id=device[way], device_id_type=MESH)

    pl.when(z > 0)(lambda: greet(DOWN))
    pl.when(z < 3)(lambda: greet(UP))
    greet(SIDE)
    greet(TWIN)

    own_blk = block_of(own)
    loads[PARTS].wait()
    for k in range(PARTS):
        loads[k].wait()
        wide = xs[own + k].astype(jnp.float32)
        a_col[pl.ds(k * part, part), :] = jnp.broadcast_to(
            scale * jnp.sum(wide * wide, axis=1, keepdims=True), (part, LANES))
    for g in range(groups):
        span = pl.ds(g * LANES, LANES)
        aq[own_blk, g:g + 1, :] = jnp.transpose(a_col[span, :])[0:1, :]
        aq[own_blk, groups + g:groups + g + 1, :] = q_ref[g:g + 1, :]
        q_col[span, :] = jnp.transpose(jnp.broadcast_to(q_ref[g:g + 1, :], (LANES, LANES)))

    pl.semaphore_wait(barrier, jnp.where(corner, 3, 4))
    for k in range(PARTS):
        send_if(z > 0, DOWN, own + k)
        send_if(z < 3, UP, own + k)
        send(SIDE, own + k)
        send(TWIN, own + k)
        if k == 0:
            aq_send_if(z > 0, DOWN, own_blk)
            aq_send_if(z < 3, UP, own_blk)
            aq_send_to(SIDE, own_blk)
            aq_send_to(TWIN, own_blk)
    force[...] = jnp.zeros_like(force)
    row_sum[...] = jnp.zeros_like(row_sum)
    e_acc[...] = jnp.zeros_like(e_acc)

    def share(ch):
        same_line = (block_of(ch) // 8) == y
        z_j = block_of(ch) % 4
        at_corner = jnp.where((z_j == z) | ((z_j == far) & same_line), 0.5, 0.0)
        at_middle = jnp.where((z_j == 1) | (z_j == 2), 0.5, 1.0)
        return jnp.where(corner, at_corner, at_middle)

    def weights_of(x_i, a_i, q_i, ch, k):
        blk = block_of(ch)
        def lanes(first):
            return jnp.concatenate([aq[blk, pl.ds(first + h, 1), :] for h in range(2)], axis=1)
        a_i, q_i = (jnp.concatenate([v] * 2, axis=1) for v in (a_i, q_i))
        dots = lax.dot_general(x_i, xs[ch], NT, preferred_element_type=jnp.float32)
        power = jnp.minimum((2.0 * scale * dots - lanes(2 * k)) - a_i, 0.0)
        return (q_i * lanes(groups + 2 * k)) * jnp.exp2(power)

    def fold(weights):
        return weights[:, :LANES] + weights[:, LANES:]

    def stack(halves):
        return jnp.sum(halves.reshape(part // 8, 8, LANES), axis=0)

    def tile(r, chunks, parts_of, masked):
        span = pl.ds(r * part, part)
        acc = force[span, :]
        total = row_sum[span, :]
        e_part = jnp.zeros((8, LANES), jnp.float32)
        for n, (ch, k) in enumerate(zip(chunks, parts_of)):
            weights = weights_of(xs[own + r], a_col[span, :], q_col[span, :], ch, k)
            if masked and n == r:
                rid = lax.broadcasted_iota(jnp.int32, weights.shape, 0)
                cid = lax.broadcasted_iota(jnp.int32, weights.shape, 1)
                weights = jnp.where(rid == cid, 0.0, weights)
            halves = fold(weights)
            total = total + halves
            e_part = e_part + share(ch) * stack(halves)
            acc = acc + jnp.dot(weights.astype(jnp.bfloat16), xs[ch], preferred_element_type=jnp.float32)
        force[span, :] = acc
        row_sum[span, :] = total
        e_acc[...] += e_part

    def pairs(chunks, parts_of, masked=False):
        for r in range(PARTS):
            tile(r, chunks, parts_of, masked)

    end_rows = chunk(y, far, 0)
    end_cols = chunk(1 - y, other, 0) + jnp.where(z == 1, 0, plane)

    def end_vectors():
        blk = block_of(end_rows)
        for g in range(groups):
            for ref, first in ((a_end, 0), (q_end, groups)):
                row = aq[blk, first + g:first + g + 1, :]
                ref[pl.ds(g * LANES, LANES), :] = jnp.transpose(jnp.broadcast_to(row, (LANES, LANES)))

    def end_energy(k):
        e_part = jnp.zeros((8, LANES), jnp.float32)
        for r in range(PARTS):
            span = pl.ds(r * part, part)
            e_part = e_part + stack(fold(weights_of(
                xs[end_rows + r], a_end[span, :], q_end[span, :], end_cols + k, k)))
        e_acc[...] += e_part

    pairs([own + k for k in range(PARTS)], range(PARTS), masked=True)
    aq_arrive(own_blk + plane // PARTS)
    for k in range(PARTS):
        arrive(own + plane + k)
    pairs([own + plane + k for k in range(2)], range(2))

    place = seg * 4 + z

    def send_energy():
        for d in range(1, 16):
            peer = (place + d) % 16
            pltpu.make_async_remote_copy(
                src_ref=es.at[place], dst_ref=es.at[place], send_sem=e_send, recv_sem=e_recv,
                device_id={'seg': peer // 4, 'col': peer % 4}, device_id_type=MESH).start()

    def cross_event(zb, k, pass_on):
        ch = chunk(1 - y, zb, k)
        arrive(ch)
        if pass_on:
            onward(zb, ch)
        send(TWIN, ch)

    def schedule(u):
        k4 = u % 4
        v = u + 8
        along_corner = jnp.where(u < 12, chunk(y, line(u // 4), k4), chunk(1 - y, line(u - 12), LAST))
        along_middle = jnp.where(u < 8, chunk(y, jnp.where(u < 4, near, far), k4),
                                 jnp.where(u == 8, chunk(1 - y, near, 2), chunk(1 - y, far, u - 9)))
        side_corner = chunk(1 - y, jnp.where(u < 13, line(v // 3 - 4), far), jnp.where(u < 13, v % 3, LAST))
        side_middle = jnp.where(
            u < 8, chunk(1 - y, jnp.where(u % 2 == 0, near, other), v // 2 - 6),
            jnp.where(u < 10, chunk(1 - y, other, u - 6), chunk(1 - y, jnp.where(u == 10, near, far), LAST)))
        side = jnp.where(u < 4, chunk(1 - y, z, u), jnp.where(corner, side_corner, side_middle))
        return jnp.where(corner, along_corner, along_middle), side

    def cross_opens(u):
        return (u == 0) | (u == 4) | (corner & ((u == 7) | (u == 10))) | (~corner & ((u == 5) | (u == 9)))

    def evaluate(chunks):
        pairs(chunks, [ch % PARTS for ch in chunks])

    def from_twin(u):
        along, side = (ch + plane for ch in schedule(u))

        @pl.when((u == 0) | (u == 4) | (corner & (u == 8)))
        def _():
            aq_arrive(block_of(along))

        @pl.when(cross_opens(u))
        def _():
            aq_arrive(block_of(jnp.where(~corner & (u == 9), along, side)))

        arrive(along)
        arrive(side)
        evaluate([along, side])

    def step(u, carry):
        @pl.when(u == 0)
        def _():
            evaluate([own + plane + 2, own + plane + 3])

        @pl.when((u > 0) & (corner | (u < 13)))
        def _():
            from_twin(u - 1)

        @pl.when(u == 12)
        def _():
            es[place] = e_acc[...]

        along, side = schedule(u)

        @pl.when(corner & (u < 12))
        def _():
            line_event(line(u // 4), u % 4)

        @pl.when(corner & (u >= 12))
        def _():
            cross_event(line(u - 12), LAST, False)

        @pl.when(~corner & (u < 4))
        def _():
            line_event(near, u)
            line_event(other, u)

        @pl.when(~corner & (u >= 4) & (u < 8))
        def _():
            line_event(far, u - 4)

        @pl.when(~corner & (u == 7))
        def _():
            ch = chunk(1 - y, z, LAST)
            send_if(z == 1, DOWN, ch)
            send_if(z == 2, UP, ch)

        @pl.when(~corner & ((u == 6) | (u == 7)))
        def _():
            cross_event(other, u - 4, True)

        @pl.when(~corner & (u == 9))
        def _():
            cross_event(near, LAST, True)

        @pl.when(~corner & (u == 11))
        def _():
            cross_event(far, 2, False)
            cross_event(far, LAST, False)

        @pl.when(corner | (u < 11))
        def _():
            ch = jnp.where(~corner & (u >= 8), along, side)
            arrive(ch)
            send(TWIN, ch)

        @pl.when((u == 3) | (corner & (u == 2)))
        def _():
            send_if(z < 2, UP, side)
            send_if(z >= 2, DOWN, side)

        @pl.when(cross_opens(u))
        def _():
            blk = block_of(jnp.where(~corner & (u == 9), along, side))
            aq_arrive(blk)
            aq_send_to(TWIN, blk)

        pl.when(u == jnp.where(corner, 12, 13))(send_energy)

        @pl.when(corner | (u < 12))
        def _():
            evaluate([along, side])

        @pl.when(~corner & ((u == 1) | (u == 3)))
        def _():
            pair = [chunk(y, other, u - 1), chunk(y, other, u)]

            @pl.when(u == 1)
            def _():
                aq_arrive(block_of(pair[0] + plane))

            for ch in pair:
                arrive(ch + plane)
            evaluate(pair + [ch + plane for ch in pair])

        pl.when(~corner & (u == 6))(end_vectors)
        pl.when(~corner & (u >= 7) & (u < 11))(lambda: end_energy(u - 7))
        return carry

    lax.fori_loop(0, 14, step, 0)
    pl.when(corner)(lambda: from_twin(13))

    def drain(sem, ref):
        pltpu.make_async_copy(ref, ref, sem).wait()

    drain(send_sem.at[TWIN], xs.at[pl.ds(0, 8 * PARTS)])

    inv_len2 = 1.0 / feat
    for r in range(PARTS):
        span = pl.ds(r * part, part)
        full = jnp.sum(row_sum[span, :], axis=1, keepdims=True)
        out_ref[span, :] = (full * xs[own + r].astype(jnp.float32) - force[span, :]) * inv_len2

    drain(aq_send.at[TWIN], aq.at[pl.ds(0, 8)])
    drain(aq_send.at[SIDE], aq.at[pl.ds(0, 4)])
    for zz, counts in enumerate(((0, 6, 14), (14, 11, 11), (11, 14, 11), (6, 0, 14))):
        @pl.when(z == zz)
        def _():
            for way, count in zip((DOWN, UP, SIDE), counts):
                if count:
                    drain(send_sem.at[way], xs.at[pl.ds(0, count)])
            if zz:
                drain(aq_send.at[DOWN], aq.at[pl.ds(0, 4 - zz)])
            if zz < 3:
                drain(aq_send.at[UP], aq.at[pl.ds(0, zz + 1)])
    drain(e_recv, es.at[pl.ds(0, 15)])
    drain(e_send, es.at[pl.ds(0, 15)])
    e_ref[0] = jnp.sum(es[...])


def solution(mesh):
    assert (mesh.shape['seg'], mesh.shape['col']) == (4, 4)

    def per_device(x_own, q_own):
        rows, feat = x_own.shape
        part = rows // PARTS
        groups = rows // LANES
        f32, bf16 = jnp.float32, jnp.bfloat16
        vmem = pltpu.VMEM
        dma = pltpu.SemaphoreType.DMA
        return pl.pallas_call(
            pair_kernel,
            out_shape=(jax.ShapeDtypeStruct((rows, feat), f32), jax.ShapeDtypeStruct((1,), f32)),
            in_specs=[pl.BlockSpec(memory_space=pltpu.HBM)] * 2,
            out_specs=(pl.BlockSpec(memory_space=vmem), pl.BlockSpec(memory_space=pltpu.SMEM)),
            scratch_shapes=[
                vmem((16 * PARTS, part, feat), bf16), vmem((16, 2 * groups, LANES), f32), vmem((16, 8, LANES), f32),
                vmem((8, LANES), f32), vmem((groups, LANES), f32),
                vmem((rows, LANES), f32), vmem((rows, LANES), f32), vmem((rows, LANES), f32), vmem((rows, LANES), f32),
                vmem((rows, feat), f32), vmem((rows, LANES), f32),
                dma((PARTS + 1,)), dma((16 * PARTS,)), dma((16,)), dma, dma((4,)), dma((4,)), dma],
            compiler_params=pltpu.CompilerParams(
                collective_id=0, has_side_effects=True, vmem_limit_bytes=40 * 2 ** 20),
        )(*(pltpu.with_memory_space_constraint(v, pltpu.HBM) for v in (x_own, q_own.reshape(groups, LANES))))

    row_spec = P(ROW_AXES, None)
    return jax.shard_map(per_device, mesh=mesh, in_specs=(row_spec, P(ROW_AXES)),
                         out_specs=(row_spec, P('sys')), check_vma=False)
```

```python
import functools
import math

import jax
import jax.numpy as jnp
from jax import lax
from jax.experimental import pallas as pl
from jax.experimental.pallas import tpu as pltpu
from jax.sharding import PartitionSpec as P

ROW_AXES = ('sys', 'seg', 'col')
MESH = pl.DeviceIdType.MESH
NT = (((1,), (1,)), ((), ()))
PARTS = 4
LANES = 128


def pair_kernel(x_hbm, q_hbm, out_ref, e_ref, xs, aq, es, e_acc, q_ref, a_col, q_col,
                a_end, q_end, force, row_sum,
                load_sem, recv_sem, aq_recv, e_recv, send_sem, aq_send, e_send):
    rows, feat = x_hbm.shape
    part = rows // PARTS
    groups = rows // LANES
    scale = 0.5 * math.log2(math.e) / feat
    z = lax.axis_index('col')
    seg = lax.axis_index('seg')
    y, c = seg // 2, seg % 2
    corner = (z == 0) | (z == 3)
    near = 1 + z % 2
    far = 3 * (1 - z // 2)
    other = 6 - z - near - far
    plane = (1 - 2 * c) * 4 * PARTS

    def line(e):
        return jnp.where(e == 0, near, jnp.where(e == 1, other, far))

    def chunk(yy, zz, k):
        return ((2 * yy + c) * 4 + zz) * PARTS + k

    def block_of(ch):
        return ch // PARTS

    own = chunk(y, z, 0)
    LAST = PARTS - 1
    DOWN, UP, SIDE, TWIN = range(4)
    device = [{'col': z - 1}, {'col': z + 1}, {'seg': 2 * (1 - y) + c}, {'seg': 2 * y + 1 - c}]

    def send(way, ch):
        pltpu.make_async_remote_copy(
            src_ref=xs.at[ch], dst_ref=xs.at[ch], send_sem=send_sem.at[way], recv_sem=recv_sem.at[ch],
            device_id=device[way], device_id_type=MESH).start()

    def send_if(cond, way, ch):
        @pl.when(cond)
        def _():
            send(way, ch)

    def arrive(ch):
        pltpu.make_async_copy(xs.at[ch], xs.at[ch], recv_sem.at[ch]).wait()

    def onward(zb, ch):
        send_if((zb > z) & (z > 0), DOWN, ch)
        send_if((zb < z) & (z < 3), UP, ch)

    def aq_send_to(way, blk):
        pltpu.make_async_remote_copy(
            src_ref=aq.at[blk], dst_ref=aq.at[blk], send_sem=aq_send.at[way], recv_sem=aq_recv.at[blk],
            device_id=device[way], device_id_type=MESH).start()

    def aq_send_if(cond, way, blk):
        @pl.when(cond)
        def _():
            aq_send_to(way, blk)

    def aq_arrive(blk):
        pltpu.make_async_copy(aq.at[blk], aq.at[blk], aq_recv.at[blk]).wait()

    def line_event(zb, k):
        ch = chunk(y, zb, k)
        arrive(ch)
        onward(zb, ch)
        near_side = jnp.where((zb == near) | (corner & (zb == other)), 3, 2)
        send_if(k < jnp.where(corner & (zb == far), PARTS, near_side), SIDE, ch)
        send(TWIN, ch)

        @pl.when(k == 0)
        def _():
            blk = block_of(ch)
            aq_arrive(blk)
            aq_send_if((zb > z) & (z > 0), DOWN, blk)
            aq_send_if((zb < z) & (z < 3), UP, blk)
            aq_send_to(SIDE, blk)
            aq_send_to(TWIN, blk)

    loads = [pltpu.make_async_copy(x_hbm.at[pl.ds(k * part, part)], xs.at[own + k], load_sem.at[k])
             for k in range(PARTS)]
    loads.append(pltpu.make_async_copy(q_hbm, q_ref, load_sem.at[PARTS]))
    for load in loads:
        load.start()
    barrier = pltpu.get_barrier_semaphore()

    def greet(way):
        pl.semaphore_signal(barrier, inc=1, device_id=device[way], device_id_type=MESH)

    pl.when(z > 0)(lambda: greet(DOWN))
    pl.when(z < 3)(lambda: greet(UP))
    greet(SIDE)
    greet(TWIN)

    own_blk = block_of(own)
    loads[PARTS].wait()
    for k in range(PARTS):
        loads[k].wait()
        wide = xs[own + k].astype(jnp.float32)
        a_col[pl.ds(k * part, part), :] = jnp.broadcast_to(
            scale * jnp.sum(wide * wide, axis=1, keepdims=True), (part, LANES))
    for g in range(groups):
        span = pl.ds(g * LANES, LANES)
        aq[own_blk, g:g + 1, :] = jnp.transpose(a_col[span, :])[0:1, :]
        aq[own_blk, groups + g:groups + g + 1, :] = q_ref[g:g + 1, :]
        q_col[span, :] = jnp.transpose(jnp.broadcast_to(q_ref[g:g + 1, :], (LANES, LANES)))

    pl.semaphore_wait(barrier, jnp.where(corner, 3, 4))
    for k in range(PARTS):
        send_if(z > 0, DOWN, own + k)
        send_if(z < 3, UP, own + k)
        send(SIDE, own + k)
        send(TWIN, own + k)
        if k == 0:
            aq_send_if(z > 0, DOWN, own_blk)
            aq_send_if(z < 3, UP, own_blk)
            aq_send_to(SIDE, own_blk)
            aq_send_to(TWIN, own_blk)
    force[...] = jnp.zeros_like(force)
    row_sum[...] = jnp.zeros_like(row_sum)
    e_acc[...] = jnp.zeros_like(e_acc)

    def share(ch):
        same_line = (block_of(ch) // 8) == y
        z_j = block_of(ch) % 4
        at_corner = jnp.where((z_j == z) | ((z_j == far) & same_line), 0.5, 0.0)
        at_middle = jnp.where((z_j == 1) | (z_j == 2), 0.5, 1.0)
        return jnp.where(corner, at_corner, at_middle)

    def weights_of(x_i, a_i, q_i, ch, k):
        blk = block_of(ch)
        def lanes(first):
            return jnp.concatenate([aq[blk, pl.ds(first + h, 1), :] for h in range(2)], axis=1)
        a_i, q_i = (jnp.concatenate([v] * 2, axis=1) for v in (a_i, q_i))
        dots = lax.dot_general(x_i, xs[ch], NT, preferred_element_type=jnp.float32)
        power = jnp.minimum((2.0 * scale * dots - lanes(2 * k)) - a_i, 0.0)
        return (q_i * lanes(groups + 2 * k)) * jnp.exp2(power)

    def fold(weights):
        return weights[:, :LANES] + weights[:, LANES:]

    def stack(halves):
        return jnp.sum(halves.reshape(part // 8, 8, LANES), axis=0)

    def tile(r, chunks, parts_of, masked):
        span = pl.ds(r * part, part)
        acc = force[span, :]
        total = row_sum[span, :]
        e_part = jnp.zeros((8, LANES), jnp.float32)
        for n, (ch, k) in enumerate(zip(chunks, parts_of)):
            weights = weights_of(xs[own + r], a_col[span, :], q_col[span, :], ch, k)
            if masked and n == r:
                rid = lax.broadcasted_iota(jnp.int32, weights.shape, 0)
                cid = lax.broadcasted_iota(jnp.int32, weights.shape, 1)
                weights = jnp.where(rid == cid, 0.0, weights)
            halves = fold(weights)
            total = total + halves
            e_part = e_part + share(ch) * stack(halves)
            acc = acc + jnp.dot(weights.astype(jnp.bfloat16), xs[ch], preferred_element_type=jnp.float32)
        force[span, :] = acc
        row_sum[span, :] = total
        e_acc[...] += e_part

    def pairs(chunks, parts_of, masked=False):
        for r in range(PARTS):
            tile(r, chunks, parts_of, masked)

    end_rows = chunk(y, far, 0)
    end_cols = chunk(1 - y, other, 0) + jnp.where(z == 1, 0, plane)

    def end_vectors():
        blk = block_of(end_rows)
        for g in range(groups):
            for ref, first in ((a_end, 0), (q_end, groups)):
                row = aq[blk, first + g:first + g + 1, :]
                ref[pl.ds(g * LANES, LANES), :] = jnp.transpose(jnp.broadcast_to(row, (LANES, LANES)))

    def end_energy(k):
        e_part = jnp.zeros((8, LANES), jnp.float32)
        for r in range(PARTS):
            span = pl.ds(r * part, part)
            e_part = e_part + stack(fold(weights_of(
                xs[end_rows + r], a_end[span, :], q_end[span, :], end_cols + k, k)))
        e_acc[...] += e_part

    pairs([own + k for k in range(PARTS)], range(PARTS), masked=True)
    aq_arrive(own_blk + plane // PARTS)
    for k in range(PARTS):
        arrive(own + plane + k)
    pairs([own + plane + k for k in range(2)], range(2))

    place = seg * 4 + z

    def send_energy():
        for d in range(1, 16):
            peer = (place + d) % 16
            pltpu.make_async_remote_copy(
                src_ref=es.at[place], dst_ref=es.at[place], send_sem=e_send, recv_sem=e_recv,
                device_id={'seg': peer // 4, 'col': peer % 4}, device_id_type=MESH).start()

    def cross_event(zb, k, pass_on):
        ch = chunk(1 - y, zb, k)
        arrive(ch)
        if pass_on:
            onward(zb, ch)
        send(TWIN, ch)

    def schedule(u):
        k4 = u % 4
        v = u + 8
        along_corner = jnp.where(u < 12, chunk(y, line(u // 4), k4), chunk(1 - y, line(u - 12), LAST))
        along_middle = jnp.where(u < 8, chunk(y, jnp.where(u < 4, near, far), k4),
                                 jnp.where(u == 8, chunk(1 - y, near, 2), chunk(1 - y, far, u - 9)))
        side_corner = chunk(1 - y, jnp.where(u < 13, line(v // 3 - 4), far), jnp.where(u < 13, v % 3, LAST))
        side_middle = jnp.where(
            u < 8, chunk(1 - y, jnp.where(u % 2 == 0, near, other), v // 2 - 6),
            jnp.where(u < 10, chunk(1 - y, other, u - 6), chunk(1 - y, jnp.where(u == 10, near, far), LAST)))
        side = jnp.where(u < 4, chunk(1 - y, z, u), jnp.where(corner, side_corner, side_middle))
        return jnp.where(corner, along_corner, along_middle), side

    def cross_opens(u):
        return (u == 0) | (u == 4) | (corner & ((u == 7) | (u == 10))) | (~corner & ((u == 5) | (u == 9)))

    def evaluate(chunks):
        pairs(chunks, [ch % PARTS for ch in chunks])

    def from_twin(u):
        along, side = (ch + plane for ch in schedule(u))

        @pl.when((u == 0) | (u == 4) | (corner & (u == 8)))
        def _():
            aq_arrive(block_of(along))

        @pl.when(cross_opens(u))
        def _():
            aq_arrive(block_of(jnp.where(~corner & (u == 9), along, side)))

        arrive(along)
        arrive(side)

    def step(u, carry):
        along, side = schedule(u)

        @pl.when(corner)
        def _():
            line_event(line(u // 4), u % 4)

        @pl.when(~corner & (u < 4))
        def _():
            line_event(near, u)
            line_event(other, u)

        @pl.when(~corner & (u >= 4) & (u < 8))
        def _():
            line_event(far, u - 4)

        @pl.when(~corner & (u == 7))
        def _():
            ch = chunk(1 - y, z, LAST)
            send_if(z == 1, DOWN, ch)
            send_if(z == 2, UP, ch)

        @pl.when(~corner & ((u == 6) | (u == 7)))
        def _():
            cross_event(other, u - 4, True)

        @pl.when(~corner & (u == 9))
        def _():
            cross_event(near, LAST, True)

        @pl.when(~corner & (u == 11))
        def _():
            cross_event(far, 2, False)
            cross_event(far, LAST, False)

        @pl.when(corner | (u < 11))
        def _():
            ch = jnp.where(~corner & (u >= 8), along, side)
            arrive(ch)
            send(TWIN, ch)

        @pl.when((u == 3) | (corner & (u == 2)))
        def _():
            send_if(z < 2, UP, side)
            send_if(z >= 2, DOWN, side)

        @pl.when(cross_opens(u))
        def _():
            blk = block_of(jnp.where(~corner & (u == 9), along, side))
            aq_arrive(blk)
            aq_send_to(TWIN, blk)

        @pl.when(u > 0)
        def _():
            from_twin(u - 1)

        before = schedule(jnp.maximum(u - 1, 0))
        evaluate([along, side] + [jnp.where(u > 0, ch, own + 2 + n) + plane for n, ch in enumerate(before)])

        @pl.when(~corner & ((u == 1) | (u == 3)))
        def _():
            pair = [chunk(y, other, u - 1), chunk(y, other, u)]

            @pl.when(u == 1)
            def _():
                aq_arrive(block_of(pair[0] + plane))

            for ch in pair:
                arrive(ch + plane)
            evaluate(pair + [ch + plane for ch in pair])

        pl.when(~corner & (u == 6))(end_vectors)
        pl.when(~corner & (u >= 7) & (u < 11))(lambda: end_energy(u - 7))
        return carry

    lax.fori_loop(0, 12, step, 0)

    def last_steps(i, carry):
        u = 11 + (i + 1) // 2
        along, side = schedule(u)
        twin = i % 2 == 0

        @pl.when(i == 1)
        def _():
            es[place] = e_acc[...]

        @pl.when(corner & ~twin)
        def _():
            cross_event(line(u - 12), LAST, False)
            arrive(side)
            send(TWIN, side)

        pl.when(i == 1)(send_energy)

        @pl.when((corner | (i == 0)) & twin)
        def _():
            from_twin(u)

        @pl.when(corner | (i == 0))
        def _():
            evaluate([ch + jnp.where(twin, plane, 0) for ch in (along, side)])

        return carry

    lax.fori_loop(0, 5, last_steps, 0)

    def drain(sem, ref):
        pltpu.make_async_copy(ref, ref, sem).wait()

    drain(send_sem.at[TWIN], xs.at[pl.ds(0, 8 * PARTS)])

    inv_len2 = 1.0 / feat
    for r in range(PARTS):
        span = pl.ds(r * part, part)
        full = jnp.sum(row_sum[span, :], axis=1, keepdims=True)
        out_ref[span, :] = (full * xs[own + r].astype(jnp.float32) - force[span, :]) * inv_len2

    drain(aq_send.at[TWIN], aq.at[pl.ds(0, 8)])
    drain(aq_send.at[SIDE], aq.at[pl.ds(0, 4)])
    for zz, counts in enumerate(((0, 6, 14), (14, 11, 11), (11, 14, 11), (6, 0, 14))):
        @pl.when(z == zz)
        def _():
            for way, count in zip((DOWN, UP, SIDE), counts):
                if count:
                    drain(send_sem.at[way], xs.at[pl.ds(0, count)])
            if zz:
                drain(aq_send.at[DOWN], aq.at[pl.ds(0, 4 - zz)])
            if zz < 3:
                drain(aq_send.at[UP], aq.at[pl.ds(0, zz + 1)])
    drain(e_recv, es.at[pl.ds(0, 15)])
    drain(e_send, es.at[pl.ds(0, 15)])
    e_ref[0] = jnp.sum(es[...])


def solution(mesh):
    assert (mesh.shape['seg'], mesh.shape['col']) == (4, 4)

    def per_device(x_own, q_own):
        rows, feat = x_own.shape
        part = rows // PARTS
        groups = rows // LANES
        f32, bf16 = jnp.float32, jnp.bfloat16
        vmem = pltpu.VMEM
        dma = pltpu.SemaphoreType.DMA
        return pl.pallas_call(
            pair_kernel,
            out_shape=(jax.ShapeDtypeStruct((rows, feat), f32), jax.ShapeDtypeStruct((1,), f32)),
            in_specs=[pl.BlockSpec(memory_space=pltpu.HBM)] * 2,
            out_specs=(pl.BlockSpec(memory_space=vmem), pl.BlockSpec(memory_space=pltpu.SMEM)),
            scratch_shapes=[
                vmem((16 * PARTS, part, feat), bf16), vmem((16, 2 * groups, LANES), f32), vmem((16, 8, LANES), f32),
                vmem((8, LANES), f32), vmem((groups, LANES), f32),
                vmem((rows, LANES), f32), vmem((rows, LANES), f32), vmem((rows, LANES), f32), vmem((rows, LANES), f32),
                vmem((rows, feat), f32), vmem((rows, LANES), f32),
                dma((PARTS + 1,)), dma((16 * PARTS,)), dma((16,)), dma, dma((4,)), dma((4,)), dma],
            compiler_params=pltpu.CompilerParams(
                collective_id=0, has_side_effects=True, vmem_limit_bytes=40 * 2 ** 20),
        )(*(pltpu.with_memory_space_constraint(v, pltpu.HBM) for v in (x_own, q_own.reshape(groups, LANES))))

    row_spec = P(ROW_AXES, None)
    return jax.shard_map(per_device, mesh=mesh, in_specs=(row_spec, P(ROW_AXES)),
                         out_specs=(row_spec, P('sys')), check_vma=False)
```

```python
import functools
import math

import jax
import jax.numpy as jnp
from jax import lax
from jax.experimental import pallas as pl
from jax.experimental.pallas import tpu as pltpu
from jax.sharding import PartitionSpec as P

ROW_AXES = ('sys', 'seg', 'col')
MESH = pl.DeviceIdType.MESH
NT = (((1,), (1,)), ((), ()))
PARTS = 4
LANES = 128


def pair_kernel(x_hbm, q_hbm, out_ref, e_ref, xs, aq, es, e_acc, q_ref, a_col, q_col,
                a_end, q_end, force, row_sum, low,
                load_sem, recv_sem, aq_recv, e_recv, send_sem, aq_send, e_send):
    rows, feat = x_hbm.shape
    part = rows // PARTS
    groups = rows // LANES
    scale = 0.5 * math.log2(math.e) / feat
    z = lax.axis_index('col')
    seg = lax.axis_index('seg')
    y, c = seg // 2, seg % 2
    corner = (z == 0) | (z == 3)
    near = 1 + z % 2
    far = 3 * (1 - z // 2)
    other = 6 - z - near - far
    plane = (1 - 2 * c) * 4 * PARTS

    def line(e):
        return jnp.where(e == 0, near, jnp.where(e == 1, other, far))

    def chunk(yy, zz, k):
        return ((2 * yy + c) * 4 + zz) * PARTS + k

    def block_of(ch):
        return ch // PARTS

    own = chunk(y, z, 0)
    LAST = PARTS - 1
    DOWN, UP, SIDE, TWIN = range(4)
    device = [{'col': z - 1}, {'col': z + 1}, {'seg': 2 * (1 - y) + c}, {'seg': 2 * y + 1 - c}]

    def send(way, ch):
        pltpu.make_async_remote_copy(
            src_ref=xs.at[ch], dst_ref=xs.at[ch], send_sem=send_sem.at[way], recv_sem=recv_sem.at[ch],
            device_id=device[way], device_id_type=MESH).start()

    def send_if(cond, way, ch):
        @pl.when(cond)
        def _():
            send(way, ch)

    def arrive(ch):
        pltpu.make_async_copy(xs.at[ch], xs.at[ch], recv_sem.at[ch]).wait()

    def onward(zb, ch):
        send_if((zb > z) & (z > 0), DOWN, ch)
        send_if((zb < z) & (z < 3), UP, ch)

    def aq_send_to(way, blk):
        pltpu.make_async_remote_copy(
            src_ref=aq.at[blk], dst_ref=aq.at[blk], send_sem=aq_send.at[way], recv_sem=aq_recv.at[blk],
            device_id=device[way], device_id_type=MESH).start()

    def aq_send_if(cond, way, blk):
        @pl.when(cond)
        def _():
            aq_send_to(way, blk)

    def aq_arrive(blk):
        pltpu.make_async_copy(aq.at[blk], aq.at[blk], aq_recv.at[blk]).wait()

    def line_event(zb, k):
        ch = chunk(y, zb, k)
        arrive(ch)
        onward(zb, ch)
        near_side = jnp.where((zb == near) | (corner & (zb == other)), 3, 2)
        send_if(k < jnp.where(corner & (zb == far), PARTS, near_side), SIDE, ch)
        send(TWIN, ch)

        @pl.when(k == 0)
        def _():
            blk = block_of(ch)
            aq_arrive(blk)
            aq_send_if((zb > z) & (z > 0), DOWN, blk)
            aq_send_if((zb < z) & (z < 3), UP, blk)
            aq_send_to(SIDE, blk)
            aq_send_to(TWIN, blk)

    loads = [pltpu.make_async_copy(x_hbm.at[pl.ds(k * part, part)], xs.at[own + k], load_sem.at[k])
             for k in range(PARTS)]
    loads.append(pltpu.make_async_copy(q_hbm, q_ref, load_sem.at[PARTS]))
    for load in loads:
        load.start()
    barrier = pltpu.get_barrier_semaphore()

    def greet(way):
        pl.semaphore_signal(barrier, inc=1, device_id=device[way], device_id_type=MESH)

    pl.when(z > 0)(lambda: greet(DOWN))
    pl.when(z < 3)(lambda: greet(UP))
    greet(SIDE)
    greet(TWIN)

    def send_own(k):
        send_if(z > 0, DOWN, own + k)
        send_if(z < 3, UP, own + k)
        send(SIDE, own + k)
        send(TWIN, own + k)

    loads[0].wait()
    pl.semaphore_wait(barrier, jnp.where(corner, 3, 4))
    send_own(0)

    own_blk = block_of(own)
    for load in loads[1:]:
        load.wait()
    wide = xs[pl.ds(own, PARTS)].reshape(rows, feat).astype(jnp.float32)
    a_col[...] = jnp.broadcast_to(scale * jnp.sum(wide * wide, axis=1, keepdims=True), (rows, LANES))
    for g in range(groups):
        span = pl.ds(g * LANES, LANES)
        aq[own_blk, g:g + 1, :] = jnp.transpose(a_col[span, :])[0:1, :]
        aq[own_blk, groups + g:groups + g + 1, :] = q_ref[g:g + 1, :]

    aq_send_if(z > 0, DOWN, own_blk)
    aq_send_if(z < 3, UP, own_blk)
    aq_send_to(SIDE, own_blk)
    aq_send_to(TWIN, own_blk)
    for k in range(1, PARTS):
        send_own(k)
    for g in range(groups):
        q_col[pl.ds(g * LANES, LANES), :] = jnp.transpose(jnp.broadcast_to(q_ref[g:g + 1, :], (LANES, LANES)))
    force[...] = jnp.zeros_like(force)
    row_sum[...] = jnp.zeros_like(row_sum)
    e_acc[...] = jnp.zeros_like(e_acc)

    def share(ch):
        z_j = block_of(ch) % 4
        at_corner = jnp.where(z_j == z, 0.5, 0.0)
        at_middle = jnp.where((z_j == 1) | (z_j == 2), 0.5, 1.0)
        return jnp.where(corner, at_corner, at_middle)

    def weights_of(x_i, a_i, q_i, ch, k):
        blk = block_of(ch)
        def lanes(first):
            return jnp.concatenate([aq[blk, pl.ds(first + h, 1), :] for h in range(2)], axis=1)
        a_i, q_i = (jnp.concatenate([v] * 2, axis=1) for v in (a_i, q_i))
        dots = lax.dot_general(x_i, xs[ch], NT, preferred_element_type=jnp.float32)
        power = jnp.minimum((2.0 * scale * dots - lanes(2 * k)) - a_i, 0.0)
        return (q_i * lanes(groups + 2 * k)) * jnp.exp2(power)

    def fold(weights):
        return weights[:, :LANES] + weights[:, LANES:]

    def stack(halves):
        return jnp.sum(halves.reshape(halves.shape[0] // 8, 8, LANES), axis=0)

    def pairs(chunks, parts_of, masked=False):
        x_own = xs[pl.ds(own, PARTS)].reshape(rows, feat)
        total = row_sum[...]
        e_part = jnp.zeros((8, LANES), jnp.float32)
        for n, (ch, k) in enumerate(zip(chunks, parts_of)):
            weights = weights_of(x_own, a_col[...], q_col[...], ch, k)
            if masked:
                rid = lax.broadcasted_iota(jnp.int32, weights.shape, 0)
                cid = lax.broadcasted_iota(jnp.int32, weights.shape, 1)
                weights = jnp.where(rid == cid + n * part, 0.0, weights)
            halves = fold(weights)
            total = total + halves
            e_part = e_part + share(ch) * stack(halves)
            low[:, pl.ds(n * part, part)] = weights.astype(jnp.bfloat16)
        row_sum[...] = total
        e_acc[...] += e_part
        acc = force[...]
        for n, ch in enumerate(chunks):
            acc = acc + jnp.dot(low[:, pl.ds(n * part, part)], xs[ch], preferred_element_type=jnp.float32)
        force[...] = acc

    end_rows = chunk(y, far, 0)
    end_cols = [chunk(yy, other, 0) + jnp.where(z == 1, 0, plane) for yy in (y, 1 - y)]

    def end_vectors():
        blk = block_of(end_rows)
        for g in range(groups):
            for ref, first in ((a_end, 0), (q_end, groups)):
                row = aq[blk, first + g:first + g + 1, :]
                ref[pl.ds(g * LANES, LANES), :] = jnp.transpose(jnp.broadcast_to(row, (LANES, LANES)))

    def end_energy(k):
        e_part = jnp.zeros((8, LANES), jnp.float32)
        x_end = xs[pl.ds(end_rows, PARTS)].reshape(rows, feat)
        for cols in end_cols:
            e_part = e_part + stack(fold(weights_of(x_end, a_end[...], q_end[...], cols + k, k)))
        e_acc[...] += e_part

    pairs([own + k for k in range(PARTS)], range(PARTS), masked=True)
    aq_arrive(own_blk + plane // PARTS)
    for k in range(PARTS):
        arrive(own + plane + k)
    pairs([own + plane + k for k in range(2)], range(2))

    place = seg * 4 + z

    def send_energy():
        for d in range(1, 16):
            peer = (place + d) % 16
            pltpu.make_async_remote_copy(
                src_ref=es.at[place], dst_ref=es.at[place], send_sem=e_send, recv_sem=e_recv,
                device_id={'seg': peer // 4, 'col': peer % 4}, device_id_type=MESH).start()

    def cross_event(zb, k, pass_on):
        ch = chunk(1 - y, zb, k)
        arrive(ch)
        if pass_on:
            onward(zb, ch)
        send(TWIN, ch)

    def schedule(u):
        k4 = u % 4
        v = u + 8
        along_corner = jnp.where(u < 12, chunk(y, line(u // 4), k4), chunk(1 - y, line(u - 12), LAST))
        along_middle = jnp.where(u < 8, chunk(y, jnp.where(u < 4, near, far), k4),
                                 jnp.where(u == 8, chunk(1 - y, near, 2), chunk(1 - y, far, u - 9)))
        side_corner = chunk(1 - y, jnp.where(u < 13, line(v // 3 - 4), far), jnp.where(u < 13, v % 3, LAST))
        side_middle = jnp.where(
            u < 8, chunk(1 - y, jnp.where(u % 2 == 0, near, other), v // 2 - 6),
            jnp.where(u < 10, chunk(1 - y, other, u - 6), chunk(1 - y, jnp.where(u == 10, near, far), LAST)))
        side = jnp.where(u < 4, chunk(1 - y, z, u), jnp.where(corner, side_corner, side_middle))
        return jnp.where(corner, along_corner, along_middle), side

    def cross_opens(u):
        return (u == 0) | (u == 4) | (corner & ((u == 7) | (u == 10))) | (~corner & ((u == 5) | (u == 9)))

    def evaluate(chunks):
        pairs(chunks, [ch % PARTS for ch in chunks])

    def from_twin(u):
        along, side = (ch + plane for ch in schedule(u))

        @pl.when((u == 0) | (u == 4) | (corner & (u == 8)))
        def _():
            aq_arrive(block_of(along))

        @pl.when(cross_opens(u))
        def _():
            aq_arrive(block_of(jnp.where(~corner & (u == 9), along, side)))

        arrive(along)
        arrive(side)

    def step(u, carry):
        along, side = schedule(u)

        @pl.when(corner)
        def _():
            line_event(line(u // 4), u % 4)

        @pl.when(~corner & (u < 4))
        def _():
            line_event(near, u)
            line_event(other, u)

        @pl.when(~corner & (u >= 4) & (u < 8))
        def _():
            line_event(far, u - 4)

        @pl.when(~corner & (u == 7))
        def _():
            ch = chunk(1 - y, z, LAST)
            send_if(z == 1, DOWN, ch)
            send_if(z == 2, UP, ch)

        @pl.when(~corner & ((u == 6) | (u == 7)))
        def _():
            cross_event(other, u - 4, True)

        @pl.when(~corner & (u == 9))
        def _():
            cross_event(near, LAST, True)

        @pl.when(~corner & (u == 11))
        def _():
            cross_event(far, 2, False)
            cross_event(far, LAST, False)

        @pl.when(corner | (u < 11))
        def _():
            ch = jnp.where(~corner & (u >= 8), along, side)
            arrive(ch)
            send(TWIN, ch)

        @pl.when((u == 3) | (corner & (u == 2)))
        def _():
            send_if(z < 2, UP, side)
            send_if(z >= 2, DOWN, side)

        @pl.when(cross_opens(u))
        def _():
            blk = block_of(jnp.where(~corner & (u == 9), along, side))
            aq_arrive(blk)
            aq_send_to(TWIN, blk)

        @pl.when(u > 0)
        def _():
            from_twin(u - 1)

        before = schedule(jnp.maximum(u - 1, 0))
        evaluate([along, side] + [jnp.where(u > 0, ch, own + 2 + n) + plane for n, ch in enumerate(before)])

        @pl.when(~corner & ((u == 1) | (u == 3)))
        def _():
            pair = [chunk(y, other, u - 1), chunk(y, other, u)]

            @pl.when(u == 1)
            def _():
                aq_arrive(block_of(pair[0] + plane))

            for ch in pair:
                arrive(ch + plane)
            evaluate(pair + [ch + plane for ch in pair])

        @pl.when(corner & (u == 6))
        def _():
            es[place] = e_acc[...]

        pl.when(corner & (u == 8))(send_energy)
        pl.when(~corner & (u == 6))(end_vectors)
        pl.when(~corner & (u >= 7) & (u < 11))(lambda: end_energy(u - 7))
        return carry

    lax.fori_loop(0, 12, step, 0)

    def last_steps(i, carry):
        u = 11 + (i + 1) // 2
        along, side = schedule(u)
        twin = i % 2 == 0

        @pl.when(~corner & (i == 1))
        def _():
            es[place] = e_acc[...]

        @pl.when(corner & ~twin)
        def _():
            cross_event(line(u - 12), LAST, False)
            arrive(side)
            send(TWIN, side)

        pl.when(~corner & (i == 1))(send_energy)

        @pl.when((corner | (i == 0)) & twin)
        def _():
            from_twin(u)

        @pl.when(corner | (i == 0))
        def _():
            evaluate([ch + jnp.where(twin, plane, 0) for ch in (along, side)])

        return carry

    lax.fori_loop(0, 5, last_steps, 0)

    def drain(sem, ref):
        pltpu.make_async_copy(ref, ref, sem).wait()

    drain(send_sem.at[TWIN], xs.at[pl.ds(0, 8 * PARTS)])

    inv_len2 = 1.0 / feat
    for r in range(PARTS):
        span = pl.ds(r * part, part)
        full = jnp.sum(row_sum[span, :], axis=1, keepdims=True)
        out_ref[span, :] = (full * xs[own + r].astype(jnp.float32) - force[span, :]) * inv_len2

    drain(aq_send.at[TWIN], aq.at[pl.ds(0, 8)])
    drain(aq_send.at[SIDE], aq.at[pl.ds(0, 4)])
    for zz, counts in enumerate(((0, 6, 14), (14, 11, 11), (11, 14, 11), (6, 0, 14))):
        @pl.when(z == zz)
        def _():
            for way, count in zip((DOWN, UP, SIDE), counts):
                if count:
                    drain(send_sem.at[way], xs.at[pl.ds(0, count)])
            if zz:
                drain(aq_send.at[DOWN], aq.at[pl.ds(0, 4 - zz)])
            if zz < 3:
                drain(aq_send.at[UP], aq.at[pl.ds(0, zz + 1)])
    drain(e_recv, es.at[pl.ds(0, 15)])
    drain(e_send, es.at[pl.ds(0, 15)])
    e_ref[0] = jnp.sum(es[...])


def solution(mesh):
    assert (mesh.shape['seg'], mesh.shape['col']) == (4, 4)

    def per_device(x_own, q_own):
        rows, feat = x_own.shape
        part = rows // PARTS
        groups = rows // LANES
        f32, bf16 = jnp.float32, jnp.bfloat16
        vmem = pltpu.VMEM
        dma = pltpu.SemaphoreType.DMA
        return pl.pallas_call(
            pair_kernel,
            out_shape=(jax.ShapeDtypeStruct((rows, feat), f32), jax.ShapeDtypeStruct((1,), f32)),
            in_specs=[pl.BlockSpec(memory_space=pltpu.HBM)] * 2,
            out_specs=(pl.BlockSpec(memory_space=vmem), pl.BlockSpec(memory_space=pltpu.SMEM)),
            scratch_shapes=[
                vmem((16 * PARTS, part, feat), bf16), vmem((16, 2 * groups, LANES), f32), vmem((16, 8, LANES), f32),
                vmem((8, LANES), f32), vmem((groups, LANES), f32),
                vmem((rows, LANES), f32), vmem((rows, LANES), f32), vmem((rows, LANES), f32), vmem((rows, LANES), f32),
                vmem((rows, feat), f32), vmem((rows, LANES), f32), vmem((rows, rows), bf16),
                dma((PARTS + 1,)), dma((16 * PARTS,)), dma((16,)), dma, dma((4,)), dma((4,)), dma],
            compiler_params=pltpu.CompilerParams(
                collective_id=0, has_side_effects=True, vmem_limit_bytes=40 * 2 ** 20),
        )(*(pltpu.with_memory_space_constraint(v, pltpu.HBM) for v in (x_own, q_own.reshape(groups, LANES))))

    row_spec = P(ROW_AXES, None)
    return jax.shard_map(per_device, mesh=mesh, in_specs=(row_spec, P(ROW_AXES)),
                         out_specs=(row_spec, P('sys')), check_vma=False)
```

```python
import functools
import math

import jax
import jax.numpy as jnp
from jax import lax
from jax.experimental import pallas as pl
from jax.experimental.pallas import tpu as pltpu
from jax.sharding import PartitionSpec as P

ROW_AXES = ('sys', 'seg', 'col')
MESH = pl.DeviceIdType.MESH
NT = (((1,), (1,)), ((), ()))
PARTS = 4
LANES = 128


def pair_kernel(x_hbm, q_hbm, out_ref, e_ref, xs, aq, es, e_acc, q_ref, a_col, q_col,
                a_end, q_end, force, row_sum, low,
                load_sem, recv_sem, aq_recv, e_recv, send_sem, aq_send, e_send):
    rows, feat = x_hbm.shape
    part = rows // PARTS
    groups = rows // LANES
    scale = 0.5 * math.log2(math.e) / feat
    z = lax.axis_index('col')
    seg = lax.axis_index('seg')
    y, c = seg // 2, seg % 2
    corner = (z == 0) | (z == 3)
    near = 1 + z % 2
    far = 3 * (1 - z // 2)
    other = 6 - z - near - far
    plane = (1 - 2 * c) * 4 * PARTS

    def line(e):
        return jnp.where(e == 0, near, jnp.where(e == 1, other, far))

    def chunk(yy, zz, k):
        return ((2 * yy + c) * 4 + zz) * PARTS + k

    def block_of(ch):
        return ch // PARTS

    own = chunk(y, z, 0)
    LAST = PARTS - 1
    DOWN, UP, SIDE, TWIN = range(4)
    device = [{'col': z - 1}, {'col': z + 1}, {'seg': 2 * (1 - y) + c}, {'seg': 2 * y + 1 - c}]

    def send(way, ch):
        pltpu.make_async_remote_copy(
            src_ref=xs.at[ch], dst_ref=xs.at[ch], send_sem=send_sem.at[way], recv_sem=recv_sem.at[ch],
            device_id=device[way], device_id_type=MESH).start()

    def send_if(cond, way, ch):
        @pl.when(cond)
        def _():
            send(way, ch)

    def arrive(ch):
        pltpu.make_async_copy(xs.at[ch], xs.at[ch], recv_sem.at[ch]).wait()

    def onward(zb, ch):
        send_if((zb > z) & (z > 0), DOWN, ch)
        send_if((zb < z) & (z < 3), UP, ch)

    def aq_send_to(way, blk):
        pltpu.make_async_remote_copy(
            src_ref=aq.at[blk], dst_ref=aq.at[blk], send_sem=aq_send.at[way], recv_sem=aq_recv.at[blk],
            device_id=device[way], device_id_type=MESH).start()

    def aq_send_if(cond, way, blk):
        @pl.when(cond)
        def _():
            aq_send_to(way, blk)

    def aq_arrive(blk):
        pltpu.make_async_copy(aq.at[blk], aq.at[blk], aq_recv.at[blk]).wait()

    def line_event(zb, k):
        ch = chunk(y, zb, k)
        arrive(ch)
        onward(zb, ch)
        limit = jnp.where(corner, jnp.where(zb == other, PARTS, 3), jnp.where(zb == near, 3, 2))
        send_if(k < limit, SIDE, ch)
        send(TWIN, ch)

        @pl.when(k == 0)
        def _():
            blk = block_of(ch)
            aq_arrive(blk)
            aq_send_if((zb > z) & (z > 0), DOWN, blk)
            aq_send_if((zb < z) & (z < 3), UP, blk)
            aq_send_to(SIDE, blk)
            aq_send_to(TWIN, blk)

    loads = [pltpu.make_async_copy(x_hbm.at[pl.ds(k * part, part)], xs.at[own + k], load_sem.at[k])
             for k in range(PARTS)]
    loads.append(pltpu.make_async_copy(q_hbm, q_ref, load_sem.at[PARTS]))
    for load in loads:
        load.start()
    barrier = pltpu.get_barrier_semaphore()

    def greet(way):
        pl.semaphore_signal(barrier, inc=1, device_id=device[way], device_id_type=MESH)

    pl.when(z > 0)(lambda: greet(DOWN))
    pl.when(z < 3)(lambda: greet(UP))
    greet(SIDE)
    greet(TWIN)

    def send_own(k):
        send_if(z > 0, DOWN, own + k)
        send_if(z < 3, UP, own + k)
        send(SIDE, own + k)
        send(TWIN, own + k)

    loads[0].wait()
    pl.semaphore_wait(barrier, jnp.where(corner, 3, 4))
    send_own(0)

    own_blk = block_of(own)
    for load in loads[1:]:
        load.wait()
    wide = xs[pl.ds(own, PARTS)].reshape(rows, feat).astype(jnp.float32)
    a_col[...] = jnp.broadcast_to(scale * jnp.sum(wide * wide, axis=1, keepdims=True), (rows, LANES))
    for g in range(groups):
        span = pl.ds(g * LANES, LANES)
        aq[own_blk, g:g + 1, :] = jnp.transpose(a_col[span, :])[0:1, :]
        aq[own_blk, groups + g:groups + g + 1, :] = q_ref[g:g + 1, :]

    aq_send_if(z > 0, DOWN, own_blk)
    aq_send_if(z < 3, UP, own_blk)
    aq_send_to(SIDE, own_blk)
    aq_send_to(TWIN, own_blk)
    for k in range(1, PARTS):
        send_own(k)
    for g in range(groups):
        q_col[pl.ds(g * LANES, LANES), :] = jnp.transpose(jnp.broadcast_to(q_ref[g:g + 1, :], (LANES, LANES)))
    force[...] = jnp.zeros_like(force)
    row_sum[...] = jnp.zeros_like(row_sum)
    e_acc[...] = jnp.zeros_like(e_acc)

    def share(ch):
        z_j = block_of(ch) % 4
        at_corner = jnp.where(z_j == z, 0.5, 0.0)
        at_middle = jnp.where((z_j == 1) | (z_j == 2), 0.5, 1.0)
        return jnp.where(corner, at_corner, at_middle)

    def weights_of(x_i, a_i, q_i, ch, k):
        blk = block_of(ch)
        def lanes(first):
            return jnp.concatenate([aq[blk, pl.ds(first + h, 1), :] for h in range(2)], axis=1)
        a_i, q_i = (jnp.concatenate([v] * 2, axis=1) for v in (a_i, q_i))
        dots = lax.dot_general(x_i, xs[ch], NT, preferred_element_type=jnp.float32)
        power = jnp.minimum((2.0 * scale * dots - lanes(2 * k)) - a_i, 0.0)
        return (q_i * lanes(groups + 2 * k)) * jnp.exp2(power)

    def fold(weights):
        return weights[:, :LANES] + weights[:, LANES:]

    def stack(halves):
        return jnp.sum(halves.reshape(halves.shape[0] // 8, 8, LANES), axis=0)

    def pairs(chunks, parts_of, masked=False):
        x_own = xs[pl.ds(own, PARTS)].reshape(rows, feat)
        total = row_sum[...]
        e_part = jnp.zeros((8, LANES), jnp.float32)
        for n, (ch, k) in enumerate(zip(chunks, parts_of)):
            weights = weights_of(x_own, a_col[...], q_col[...], ch, k)
            if masked:
                rid = lax.broadcasted_iota(jnp.int32, weights.shape, 0)
                cid = lax.broadcasted_iota(jnp.int32, weights.shape, 1)
                weights = jnp.where(rid == cid + n * part, 0.0, weights)
            halves = fold(weights)
            total = total + halves
            e_part = e_part + share(ch) * stack(halves)
            low[:, pl.ds(n * part, part)] = weights.astype(jnp.bfloat16)
        row_sum[...] = total
        e_acc[...] += e_part
        acc = force[...]
        for n, ch in enumerate(chunks):
            acc = acc + jnp.dot(low[:, pl.ds(n * part, part)], xs[ch], preferred_element_type=jnp.float32)
        force[...] = acc

    end_rows = chunk(y, far, 0)
    end_cols = [chunk(yy, other, 0) + jnp.where(z == 1, 0, plane) for yy in (y, 1 - y)]

    def end_vectors():
        blk = block_of(end_rows)
        for g in range(groups):
            for ref, first in ((a_end, 0), (q_end, groups)):
                row = aq[blk, first + g:first + g + 1, :]
                ref[pl.ds(g * LANES, LANES), :] = jnp.transpose(jnp.broadcast_to(row, (LANES, LANES)))

    def end_energy(k):
        e_part = jnp.zeros((8, LANES), jnp.float32)
        x_end = xs[pl.ds(end_rows, PARTS)].reshape(rows, feat)
        for cols in end_cols:
            e_part = e_part + stack(fold(weights_of(x_end, a_end[...], q_end[...], cols + k, k)))
        e_acc[...] += e_part

    pairs([own + k for k in range(PARTS)], range(PARTS), masked=True)
    aq_arrive(own_blk + plane // PARTS)
    for k in range(PARTS):
        arrive(own + plane + k)
    pairs([own + plane + k for k in range(2)], range(2))

    place = seg * 4 + z

    def send_energy():
        for d in range(1, 16):
            peer = (place + d) % 16
            pltpu.make_async_remote_copy(
                src_ref=es.at[place], dst_ref=es.at[place], send_sem=e_send, recv_sem=e_recv,
                device_id={'seg': peer // 4, 'col': peer % 4}, device_id_type=MESH).start()

    def cross_event(zb, k, pass_on):
        ch = chunk(1 - y, zb, k)
        arrive(ch)
        if pass_on:
            onward(zb, ch)
        send(TWIN, ch)

    def schedule(u):
        k4 = u % 4
        along_corner = jnp.where(u < 12, chunk(y, line(u // 4), k4), chunk(1 - y, jnp.where(u == 12, near, far), LAST))
        along_middle = jnp.where(u < 8, chunk(y, jnp.where(u < 4, near, far), k4),
                                 jnp.where(u == 8, chunk(1 - y, near, 2), chunk(1 - y, far, u - 9)))
        side_corner = jnp.where(u < 7, chunk(1 - y, near, u - 4),
                                jnp.where(u < 11, chunk(1 - y, other, u - 7), chunk(1 - y, far, u - 11)))
        side_middle = jnp.where(
            u < 8, chunk(1 - y, jnp.where(u % 2 == 0, near, other), u // 2 - 2),
            jnp.where(u < 10, chunk(1 - y, other, u - 6), chunk(1 - y, jnp.where(u == 10, near, far), LAST)))
        side = jnp.where(u < 4, chunk(1 - y, z, u), jnp.where(corner, side_corner, side_middle))
        return jnp.where(corner, along_corner, along_middle), side

    def cross_opens(u):
        return (u == 0) | (u == 4) | (corner & ((u == 7) | (u == 11))) | (~corner & ((u == 5) | (u == 9)))

    def evaluate(chunks):
        pairs(chunks, [ch % PARTS for ch in chunks])

    def from_twin(u):
        along, side = (ch + plane for ch in schedule(u))

        @pl.when((u == 0) | (u == 4) | (corner & (u == 8)))
        def _():
            aq_arrive(block_of(along))

        @pl.when(cross_opens(u))
        def _():
            aq_arrive(block_of(jnp.where(~corner & (u == 9), along, side)))

        arrive(along)
        arrive(side)

    def step(u, carry):
        along, side = schedule(u)

        @pl.when(corner)
        def _():
            line_event(line(u // 4), u % 4)

        @pl.when(~corner & (u < 4))
        def _():
            line_event(near, u)
            line_event(other, u)

        @pl.when(~corner & (u >= 4) & (u < 8))
        def _():
            line_event(far, u - 4)

        @pl.when(~corner & (u == 7))
        def _():
            ch = chunk(1 - y, z, LAST)
            send_if(z == 1, DOWN, ch)
            send_if(z == 2, UP, ch)

        @pl.when(~corner & ((u == 6) | (u == 7)))
        def _():
            cross_event(other, u - 4, True)

        @pl.when(~corner & (u == 9))
        def _():
            cross_event(near, LAST, False)

        @pl.when(~corner & (u == 11))
        def _():
            cross_event(far, 2, False)

        @pl.when(corner | (u < 11))
        def _():
            ch = jnp.where(~corner & (u >= 8), along, side)
            arrive(ch)
            send(TWIN, ch)

        @pl.when(~corner & (u == 10))
        def _():
            cross_event(far, LAST, True)

        @pl.when((u == 3) | (corner & (u == 2)))
        def _():
            send_if(z < 2, UP, side)
            send_if(z >= 2, DOWN, side)

        @pl.when(cross_opens(u))
        def _():
            blk = block_of(jnp.where(~corner & (u == 9), along, side))
            aq_arrive(blk)
            aq_send_to(TWIN, blk)

        @pl.when(u > 0)
        def _():
            from_twin(u - 1)

        before = schedule(jnp.maximum(u - 1, 0))
        evaluate([along, side] + [jnp.where(u > 0, ch, own + 2 + n) + plane for n, ch in enumerate(before)])

        @pl.when(~corner & ((u == 1) | (u == 3)))
        def _():
            pair = [chunk(y, other, u - 1), chunk(y, other, u)]

            @pl.when(u == 1)
            def _():
                aq_arrive(block_of(pair[0] + plane))

            for ch in pair:
                arrive(ch + plane)
            evaluate(pair + [ch + plane for ch in pair])

        @pl.when(corner & (u == 6))
        def _():
            es[place] = e_acc[...]

        pl.when(corner & (u == 8))(send_energy)
        pl.when(~corner & (u == 6))(end_vectors)
        pl.when(~corner & (u >= 7) & (u < 11))(lambda: end_energy(u - 7))
        return carry

    lax.fori_loop(0, 12, step, 0)

    def last_steps(i, carry):
        @pl.when(~corner & (i == 1))
        def _():
            es[place] = e_acc[...]

        @pl.when(corner & (i > 0))
        def _():
            cross_event(jnp.where(i == 1, near, far), LAST, False)
            side = schedule(11 + i)[1]
            arrive(side)
            send(TWIN, side)

        pl.when(~corner & (i == 1))(send_energy)

        @pl.when(corner | (i == 0))
        def _():
            @pl.when(i == 0)
            def _():
                from_twin(11)

            @pl.when(i == 2)
            def _():
                from_twin(12)
                evaluate(list(schedule(13)) + [ch + plane for ch in schedule(12)])
                from_twin(13)

            u = jnp.where(i == 0, 11, 11 + i)
            evaluate([ch + jnp.where(i == 1, 0, plane) for ch in schedule(u)])

        return carry

    lax.fori_loop(0, 3, last_steps, 0)

    def drain(sem, ref):
        pltpu.make_async_copy(ref, ref, sem).wait()

    drain(send_sem.at[TWIN], xs.at[pl.ds(0, 8 * PARTS)])

    inv_len2 = 1.0 / feat
    for r in range(PARTS):
        span = pl.ds(r * part, part)
        full = jnp.sum(row_sum[span, :], axis=1, keepdims=True)
        out_ref[span, :] = (full * xs[own + r].astype(jnp.float32) - force[span, :]) * inv_len2

    drain(aq_send.at[TWIN], aq.at[pl.ds(0, 8)])
    drain(aq_send.at[SIDE], aq.at[pl.ds(0, 4)])
    for zz, counts in enumerate(((0, 6, 14), (14, 11, 11), (11, 14, 11), (6, 0, 14))):
        @pl.when(z == zz)
        def _():
            for way, count in zip((DOWN, UP, SIDE), counts):
                if count:
                    drain(send_sem.at[way], xs.at[pl.ds(0, count)])
            if zz:
                drain(aq_send.at[DOWN], aq.at[pl.ds(0, 4 - zz)])
            if zz < 3:
                drain(aq_send.at[UP], aq.at[pl.ds(0, zz + 1)])
    drain(e_recv, es.at[pl.ds(0, 15)])
    drain(e_send, es.at[pl.ds(0, 15)])
    e_ref[0] = jnp.sum(es[...])


def solution(mesh):
    assert (mesh.shape['seg'], mesh.shape['col']) == (4, 4)

    def per_device(x_own, q_own):
        rows, feat = x_own.shape
        part = rows // PARTS
        groups = rows // LANES
        f32, bf16 = jnp.float32, jnp.bfloat16
        vmem = pltpu.VMEM
        dma = pltpu.SemaphoreType.DMA
        return pl.pallas_call(
            pair_kernel,
            out_shape=(jax.ShapeDtypeStruct((rows, feat), f32), jax.ShapeDtypeStruct((1,), f32)),
            in_specs=[pl.BlockSpec(memory_space=pltpu.HBM)] * 2,
            out_specs=(pl.BlockSpec(memory_space=vmem), pl.BlockSpec(memory_space=pltpu.SMEM)),
            scratch_shapes=[
                vmem((16 * PARTS, part, feat), bf16), vmem((16, 2 * groups, LANES), f32), vmem((16, 8, LANES), f32),
                vmem((8, LANES), f32), vmem((groups, LANES), f32),
                vmem((rows, LANES), f32), vmem((rows, LANES), f32), vmem((rows, LANES), f32), vmem((rows, LANES), f32),
                vmem((rows, feat), f32), vmem((rows, LANES), f32), vmem((rows, rows), bf16),
                dma((PARTS + 1,)), dma((16 * PARTS,)), dma((16,)), dma, dma((4,)), dma((4,)), dma],
            compiler_params=pltpu.CompilerParams(
                collective_id=0, has_side_effects=True, vmem_limit_bytes=40 * 2 ** 20),
        )(*(pltpu.with_memory_space_constraint(v, pltpu.HBM) for v in (x_own, q_own.reshape(groups, LANES))))

    row_spec = P(ROW_AXES, None)
    return jax.shard_map(per_device, mesh=mesh, in_specs=(row_spec, P(ROW_AXES)),
                         out_specs=(row_spec, P('sys')), check_vma=False)
```

```python
import functools
import math

import jax
import jax.numpy as jnp
from jax import lax
from jax.experimental import pallas as pl
from jax.experimental.pallas import tpu as pltpu
from jax.sharding import PartitionSpec as P

ROW_AXES = ('sys', 'seg', 'col')
MESH = pl.DeviceIdType.MESH
NT = (((1,), (1,)), ((), ()))
PARTS = 4
LANES = 128


def pair_kernel(x_hbm, q_hbm, out_ref, e_ref, xs, aq, es, e_acc, q_ref, a_col, q_col,
                a_end, q_end, force, row_sum, low,
                load_sem, recv_sem, aq_recv, e_recv, send_sem, aq_send, e_send):
    rows, feat = x_hbm.shape
    part = rows // PARTS
    groups = rows // LANES
    scale = 0.5 * math.log2(math.e) / feat
    z = lax.axis_index('col')
    seg = lax.axis_index('seg')
    y, c = seg // 2, seg % 2
    corner = (z == 0) | (z == 3)
    near = 1 + z % 2
    far = 3 * (1 - z // 2)
    other = 6 - z - near - far
    plane = (1 - 2 * c) * 4 * PARTS

    def line(e):
        return jnp.where(e == 0, near, jnp.where(e == 1, other, far))

    def chunk(yy, zz, k):
        return ((2 * yy + c) * 4 + zz) * PARTS + k

    def block_of(ch):
        return ch // PARTS

    own = chunk(y, z, 0)
    LAST = PARTS - 1
    DOWN, UP, SIDE, TWIN = range(4)
    device = [{'col': z - 1}, {'col': z + 1}, {'seg': 2 * (1 - y) + c}, {'seg': 2 * y + 1 - c}]

    def send(way, ch):
        pltpu.make_async_remote_copy(
            src_ref=xs.at[ch], dst_ref=xs.at[ch], send_sem=send_sem.at[way], recv_sem=recv_sem.at[ch],
            device_id=device[way], device_id_type=MESH).start()

    def send_if(cond, way, ch):
        @pl.when(cond)
        def _():
            send(way, ch)

    def arrive(ch):
        pltpu.make_async_copy(xs.at[ch], xs.at[ch], recv_sem.at[ch]).wait()

    def onward(zb, ch):
        send_if((zb > z) & (z > 0), DOWN, ch)
        send_if((zb < z) & (z < 3), UP, ch)

    def aq_send_to(way, blk):
        pltpu.make_async_remote_copy(
            src_ref=aq.at[blk], dst_ref=aq.at[blk], send_sem=aq_send.at[way], recv_sem=aq_recv.at[blk],
            device_id=device[way], device_id_type=MESH).start()

    def aq_send_if(cond, way, blk):
        @pl.when(cond)
        def _():
            aq_send_to(way, blk)

    def aq_arrive(blk):
        pltpu.make_async_copy(aq.at[blk], aq.at[blk], aq_recv.at[blk]).wait()

    def line_event(zb, k):
        ch = chunk(y, zb, k)
        arrive(ch)
        onward(zb, ch)
        limit = jnp.where(corner, jnp.where(zb == other, PARTS, 3), jnp.where(zb == near, 3, 2))
        send_if(k < limit, SIDE, ch)
        send(TWIN, ch)

        @pl.when(k == 0)
        def _():
            blk = block_of(ch)
            aq_arrive(blk)
            aq_send_if((zb > z) & (z > 0), DOWN, blk)
            aq_send_if((zb < z) & (z < 3), UP, blk)
            aq_send_to(SIDE, blk)
            aq_send_to(TWIN, blk)

    loads = [pltpu.make_async_copy(x_hbm.at[pl.ds(k * part, part)], xs.at[own + k], load_sem.at[k])
             for k in range(PARTS)]
    loads.append(pltpu.make_async_copy(q_hbm, q_ref, load_sem.at[PARTS]))
    for load in loads:
        load.start()
    barrier = pltpu.get_barrier_semaphore()

    def greet(way):
        pl.semaphore_signal(barrier, inc=1, device_id=device[way], device_id_type=MESH)

    pl.when(z > 0)(lambda: greet(DOWN))
    pl.when(z < 3)(lambda: greet(UP))
    greet(SIDE)
    greet(TWIN)

    def send_own(k):
        send_if(z > 0, DOWN, own + k)
        send_if(z < 3, UP, own + k)
        send(SIDE, own + k)
        send(TWIN, own + k)

    loads[0].wait()
    pl.semaphore_wait(barrier, jnp.where(corner, 3, 4))
    send_own(0)

    own_blk = block_of(own)
    for load in loads[1:]:
        load.wait()
    wide = xs[pl.ds(own, PARTS)].reshape(rows, feat).astype(jnp.float32)
    a_col[...] = jnp.broadcast_to(scale * jnp.sum(wide * wide, axis=1, keepdims=True), (rows, LANES))
    for g in range(groups):
        span = pl.ds(g * LANES, LANES)
        aq[own_blk, g:g + 1, :] = jnp.transpose(a_col[span, :])[0:1, :]
        aq[own_blk, groups + g:groups + g + 1, :] = q_ref[g:g + 1, :]

    aq_send_if(z > 0, DOWN, own_blk)
    aq_send_if(z < 3, UP, own_blk)
    aq_send_to(SIDE, own_blk)
    aq_send_to(TWIN, own_blk)
    for k in range(1, PARTS):
        send_own(k)
    for g in range(groups):
        q_col[pl.ds(g * LANES, LANES), :] = jnp.transpose(jnp.broadcast_to(q_ref[g:g + 1, :], (LANES, LANES)))
    force[...] = jnp.zeros_like(force)
    row_sum[...] = jnp.zeros_like(row_sum)
    e_acc[...] = jnp.zeros_like(e_acc)

    def share(ch):
        z_j = block_of(ch) % 4
        at_corner = jnp.where(z_j == z, 0.5, 0.0)
        at_middle = jnp.where((z_j == 1) | (z_j == 2), 0.5, 1.0)
        return jnp.where(corner, at_corner, at_middle)

    def weights_of(x_i, a_i, q_i, ch, k):
        blk = block_of(ch)
        def lanes(first):
            return jnp.concatenate([aq[blk, pl.ds(first + h, 1), :] for h in range(2)], axis=1)
        a_i, q_i = (jnp.concatenate([v] * 2, axis=1) for v in (a_i, q_i))
        dots = lax.dot_general(x_i, xs[ch], NT, preferred_element_type=jnp.float32)
        power = jnp.minimum((2.0 * scale * dots - lanes(2 * k)) - a_i, 0.0)
        return (q_i * lanes(groups + 2 * k)) * jnp.exp2(power)

    def fold(weights):
        return weights[:, :LANES] + weights[:, LANES:]

    def stack(halves):
        return jnp.sum(halves.reshape(halves.shape[0] // 8, 8, LANES), axis=0)

    def pairs(chunks, parts_of, masked=False):
        x_own = xs[pl.ds(own, PARTS)].reshape(rows, feat)
        total = row_sum[...]
        e_part = jnp.zeros((8, LANES), jnp.float32)
        for n, (ch, k) in enumerate(zip(chunks, parts_of)):
            weights = weights_of(x_own, a_col[...], q_col[...], ch, k)
            if masked:
                rid = lax.broadcasted_iota(jnp.int32, weights.shape, 0)
                cid = lax.broadcasted_iota(jnp.int32, weights.shape, 1)
                weights = jnp.where(rid == cid + n * part, 0.0, weights)
            halves = fold(weights)
            total = total + halves
            part_of_e = share(ch)
            e_part = e_part + jnp.where(part_of_e > 0.0, part_of_e * stack(halves), 0.0)
            low[:, pl.ds(n * part, part)] = weights.astype(jnp.bfloat16)
        row_sum[...] = total
        e_acc[...] += e_part
        acc = force[...]
        for n, ch in enumerate(chunks):
            acc = acc + jnp.dot(low[:, pl.ds(n * part, part)], xs[ch], preferred_element_type=jnp.float32)
        force[...] = acc

    end_rows = chunk(y, far, 0)
    end_cols = [chunk(yy, other, 0) + jnp.where(z == 1, 0, plane) for yy in (y, 1 - y)]

    def end_vectors():
        blk = block_of(end_rows)
        for g in range(groups):
            for ref, first in ((a_end, 0), (q_end, groups)):
                row = aq[blk, first + g:first + g + 1, :]
                ref[pl.ds(g * LANES, LANES), :] = jnp.transpose(jnp.broadcast_to(row, (LANES, LANES)))

    def end_energy(k):
        e_part = jnp.zeros((8, LANES), jnp.float32)
        x_end = xs[pl.ds(end_rows, PARTS)].reshape(rows, feat)
        for cols in end_cols:
            e_part = e_part + stack(fold(weights_of(x_end, a_end[...], q_end[...], cols + k, k)))
        e_acc[...] += e_part

    pairs([own + k for k in range(PARTS)], range(PARTS), masked=True)
    aq_arrive(own_blk + plane // PARTS)
    for k in range(PARTS):
        arrive(own + plane + k)
    pairs([own + plane + k for k in range(2)], range(2))

    place = seg * 4 + z

    def send_energy():
        for d in range(1, 16):
            peer = (place + d) % 16
            pltpu.make_async_remote_copy(
                src_ref=es.at[place], dst_ref=es.at[place], send_sem=e_send, recv_sem=e_recv,
                device_id={'seg': peer // 4, 'col': peer % 4}, device_id_type=MESH).start()

    def cross_event(zb, k, pass_on):
        ch = chunk(1 - y, zb, k)
        arrive(ch)
        if pass_on:
            onward(zb, ch)
        send(TWIN, ch)

    def schedule(u):
        k4 = u % 4
        along_corner = jnp.where(u < 12, chunk(y, line(u // 4), k4), chunk(1 - y, jnp.where(u == 12, near, far), LAST))
        along_middle = jnp.where(u < 8, chunk(y, jnp.where(u < 4, near, far), k4),
                                 jnp.where(u == 8, chunk(1 - y, near, 2), chunk(1 - y, far, u - 9)))
        side_corner = jnp.where(u < 7, chunk(1 - y, near, u - 4),
                                jnp.where(u < 11, chunk(1 - y, other, u - 7), chunk(1 - y, far, u - 11)))
        side_middle = jnp.where(
            u < 8, chunk(1 - y, jnp.where(u % 2 == 0, near, other), u // 2 - 2),
            jnp.where(u < 10, chunk(1 - y, other, u - 6), chunk(1 - y, jnp.where(u == 10, near, far), LAST)))
        side = jnp.where(u < 4, chunk(1 - y, z, u), jnp.where(corner, side_corner, side_middle))
        return jnp.where(corner, along_corner, along_middle), side

    def cross_opens(u):
        return (u == 0) | (u == 4) | (corner & ((u == 7) | (u == 11))) | (~corner & ((u == 5) | (u == 9)))

    def evaluate(chunks):
        pairs(chunks, [ch % PARTS for ch in chunks])

    def from_twin(u):
        along, side = (ch + plane for ch in schedule(u))

        @pl.when((u == 0) | (u == 4) | (corner & (u == 8)))
        def _():
            aq_arrive(block_of(along))

        @pl.when(cross_opens(u))
        def _():
            aq_arrive(block_of(jnp.where(~corner & (u == 9), along, side)))

        arrive(along)
        arrive(side)

    def step(u, carry):
        along, side = schedule(u)

        @pl.when(corner)
        def _():
            line_event(line(u // 4), u % 4)

        @pl.when(~corner & (u < 4))
        def _():
            line_event(near, u)
            line_event(other, u)

        @pl.when(~corner & (u >= 4) & (u < 8))
        def _():
            line_event(far, u - 4)

        @pl.when(~corner & (u == 7))
        def _():
            ch = chunk(1 - y, z, LAST)
            send_if(z == 1, DOWN, ch)
            send_if(z == 2, UP, ch)

        @pl.when(~corner & ((u == 6) | (u == 7)))
        def _():
            cross_event(other, u - 4, True)

        @pl.when(~corner & (u == 9))
        def _():
            cross_event(near, LAST, False)

        @pl.when(~corner & (u == 11))
        def _():
            cross_event(far, 2, False)

        @pl.when(corner | (u < 11))
        def _():
            ch = jnp.where(~corner & (u >= 8), along, side)
            arrive(ch)
            send(TWIN, ch)

        @pl.when(~corner & (u == 10))
        def _():
            cross_event(far, LAST, True)

        @pl.when((u == 3) | (corner & (u == 2)))
        def _():
            send_if(z < 2, UP, side)
            send_if(z >= 2, DOWN, side)

        @pl.when(cross_opens(u))
        def _():
            blk = block_of(jnp.where(~corner & (u == 9), along, side))
            aq_arrive(blk)
            aq_send_to(TWIN, blk)

        @pl.when(u > 0)
        def _():
            from_twin(u - 1)

        before = schedule(jnp.maximum(u - 1, 0))
        evaluate([along, side] + [jnp.where(u > 0, ch, own + 2 + n) + plane for n, ch in enumerate(before)])

        @pl.when(~corner & ((u == 1) | (u == 3)))
        def _():
            pair = [chunk(y, other, u - 1), chunk(y, other, u)]

            @pl.when(u == 1)
            def _():
                aq_arrive(block_of(pair[0] + plane))

            for ch in pair:
                arrive(ch + plane)
            evaluate(pair + [ch + plane for ch in pair])

        @pl.when(corner & (u == 6))
        def _():
            es[place] = e_acc[...]

        pl.when(corner & (u == 8))(send_energy)
        pl.when(~corner & (u == 6))(end_vectors)
        pl.when(~corner & (u >= 7) & (u < 11))(lambda: end_energy(u - 7))
        return carry

    lax.fori_loop(0, 12, step, 0)

    def last_steps(i, carry):
        @pl.when(~corner & (i == 1))
        def _():
            es[place] = e_acc[...]

        @pl.when(corner & (i > 0))
        def _():
            cross_event(jnp.where(i == 1, near, far), LAST, False)
            side = schedule(11 + i)[1]
            arrive(side)
            send(TWIN, side)

        pl.when(~corner & (i == 1))(send_energy)

        @pl.when(corner | (i == 0))
        def _():
            @pl.when(i == 0)
            def _():
                from_twin(11)

            @pl.when(i == 2)
            def _():
                from_twin(12)
                evaluate(list(schedule(13)) + [ch + plane for ch in schedule(12)])
                from_twin(13)

            u = jnp.where(i == 0, 11, 11 + i)
            evaluate([ch + jnp.where(i == 1, 0, plane) for ch in schedule(u)])

        return carry

    lax.fori_loop(0, 3, last_steps, 0)

    def drain(sem, ref):
        pltpu.make_async_copy(ref, ref, sem).wait()

    drain(send_sem.at[TWIN], xs.at[pl.ds(0, 8 * PARTS)])

    inv_len2 = 1.0 / feat
    for r in range(PARTS):
        span = pl.ds(r * part, part)
        full = jnp.sum(row_sum[span, :], axis=1, keepdims=True)
        out_ref[span, :] = (full * xs[own + r].astype(jnp.float32) - force[span, :]) * inv_len2

    drain(aq_send.at[TWIN], aq.at[pl.ds(0, 8)])
    drain(aq_send.at[SIDE], aq.at[pl.ds(0, 4)])
    for zz, counts in enumerate(((0, 6, 14), (14, 11, 11), (11, 14, 11), (6, 0, 14))):
        @pl.when(z == zz)
        def _():
            for way, count in zip((DOWN, UP, SIDE), counts):
                if count:
                    drain(send_sem.at[way], xs.at[pl.ds(0, count)])
            if zz:
                drain(aq_send.at[DOWN], aq.at[pl.ds(0, 4 - zz)])
            if zz < 3:
                drain(aq_send.at[UP], aq.at[pl.ds(0, zz + 1)])
    drain(e_recv, es.at[pl.ds(0, 15)])
    drain(e_send, es.at[pl.ds(0, 15)])
    e_ref[0] = jnp.sum(es[...])


def solution(mesh):
    assert (mesh.shape['seg'], mesh.shape['col']) == (4, 4)

    def per_device(x_own, q_own):
        rows, feat = x_own.shape
        part = rows // PARTS
        groups = rows // LANES
        f32, bf16 = jnp.float32, jnp.bfloat16
        vmem = pltpu.VMEM
        dma = pltpu.SemaphoreType.DMA
        return pl.pallas_call(
            pair_kernel,
            out_shape=(jax.ShapeDtypeStruct((rows, feat), f32), jax.ShapeDtypeStruct((1,), f32)),
            in_specs=[pl.BlockSpec(memory_space=pltpu.HBM)] * 2,
            out_specs=(pl.BlockSpec(memory_space=vmem), pl.BlockSpec(memory_space=pltpu.SMEM)),
            scratch_shapes=[
                vmem((16 * PARTS, part, feat), bf16), vmem((16, 2 * groups, LANES), f32), vmem((16, 8, LANES), f32),
                vmem((8, LANES), f32), vmem((groups, LANES), f32),
                vmem((rows, LANES), f32), vmem((rows, LANES), f32), vmem((rows, LANES), f32), vmem((rows, LANES), f32),
                vmem((rows, feat), f32), vmem((rows, LANES), f32), vmem((rows, rows), bf16),
                dma((PARTS + 1,)), dma((16 * PARTS,)), dma((16,)), dma, dma((4,)), dma((4,)), dma],
            compiler_params=pltpu.CompilerParams(
                collective_id=0, has_side_effects=True, vmem_limit_bytes=40 * 2 ** 20),
        )(*(pltpu.with_memory_space_constraint(v, pltpu.HBM) for v in (x_own, q_own.reshape(groups, LANES))))

    row_spec = P(ROW_AXES, None)
    return jax.shard_map(per_device, mesh=mesh, in_specs=(row_spec, P(ROW_AXES)),
                         out_specs=(row_spec, P('sys')), check_vma=False)
```

```python
import functools
import math

import jax
import jax.numpy as jnp
from jax import lax
from jax.experimental import pallas as pl
from jax.experimental.pallas import tpu as pltpu
from jax.sharding import PartitionSpec as P

ROW_AXES = ('sys', 'seg', 'col')
MESH = pl.DeviceIdType.MESH
NT = (((1,), (1,)), ((), ()))
PARTS = 4
LANES = 128


def pair_kernel(x_hbm, q_hbm, out_ref, e_ref, xs, aq, es, e_acc, q_ref, a_col, q_col,
                a_end, q_end, force, row_sum, low,
                load_sem, recv_sem, aq_recv, e_recv, send_sem, aq_send, e_send):
    rows, feat = x_hbm.shape
    part = rows // PARTS
    groups = rows // LANES
    scale = 0.5 * math.log2(math.e) / feat
    z = lax.axis_index('col')
    seg = lax.axis_index('seg')
    y, c = seg // 2, seg % 2
    corner = (z == 0) | (z == 3)
    near = 1 + z % 2
    far = 3 * (1 - z // 2)
    other = 6 - z - near - far
    plane = (1 - 2 * c) * 4 * PARTS

    def line(e):
        return jnp.where(e == 0, near, jnp.where(e == 1, other, far))

    def chunk(yy, zz, k):
        return ((2 * yy + c) * 4 + zz) * PARTS + k

    def block_of(ch):
        return ch // PARTS

    own = chunk(y, z, 0)
    LAST = PARTS - 1
    DOWN, UP, SIDE, TWIN = range(4)
    device = [{'col': z - 1}, {'col': z + 1}, {'seg': 2 * (1 - y) + c}, {'seg': 2 * y + 1 - c}]

    def send(way, ch):
        pltpu.make_async_remote_copy(
            src_ref=xs.at[ch], dst_ref=xs.at[ch], send_sem=send_sem.at[way], recv_sem=recv_sem.at[ch],
            device_id=device[way], device_id_type=MESH).start()

    def send_if(cond, way, ch):
        @pl.when(cond)
        def _():
            send(way, ch)

    def arrive(ch):
        pltpu.make_async_copy(xs.at[ch], xs.at[ch], recv_sem.at[ch]).wait()

    def onward(zb, ch):
        send_if((zb > z) & (z > 0), DOWN, ch)
        send_if((zb < z) & (z < 3), UP, ch)

    def aq_send_to(way, blk):
        pltpu.make_async_remote_copy(
            src_ref=aq.at[blk], dst_ref=aq.at[blk], send_sem=aq_send.at[way], recv_sem=aq_recv.at[blk],
            device_id=device[way], device_id_type=MESH).start()

    def aq_send_if(cond, way, blk):
        @pl.when(cond)
        def _():
            aq_send_to(way, blk)

    def aq_arrive(blk):
        pltpu.make_async_copy(aq.at[blk], aq.at[blk], aq_recv.at[blk]).wait()

    def line_event(zb, k):
        ch = chunk(y, zb, k)
        arrive(ch)
        onward(zb, ch)
        limit = jnp.where(corner, jnp.where(zb == other, PARTS, 3), jnp.where(zb == near, 3, 2))
        send_if(k < limit, SIDE, ch)
        send(TWIN, ch)

        @pl.when(k == 0)
        def _():
            blk = block_of(ch)
            aq_arrive(blk)
            aq_send_if((zb > z) & (z > 0), DOWN, blk)
            aq_send_if((zb < z) & (z < 3), UP, blk)
            aq_send_to(SIDE, blk)
            aq_send_to(TWIN, blk)

    loads = [pltpu.make_async_copy(x_hbm.at[pl.ds(k * part, part)], xs.at[own + k], load_sem.at[k])
             for k in range(PARTS)]
    loads.append(pltpu.make_async_copy(q_hbm, q_ref, load_sem.at[PARTS]))
    for load in loads:
        load.start()
    barrier = pltpu.get_barrier_semaphore()

    def greet(way):
        pl.semaphore_signal(barrier, inc=1, device_id=device[way], device_id_type=MESH)

    pl.when(z > 0)(lambda: greet(DOWN))
    pl.when(z < 3)(lambda: greet(UP))
    greet(SIDE)
    greet(TWIN)

    def send_own(k):
        send_if(z > 0, DOWN, own + k)
        send_if(z < 3, UP, own + k)
        send(SIDE, own + k)
        send(TWIN, own + k)

    loads[0].wait()
    pl.semaphore_wait(barrier, jnp.where(corner, 3, 4))
    send_own(0)

    own_blk = block_of(own)
    for load in loads[1:]:
        load.wait()
    wide = xs[pl.ds(own, PARTS)].reshape(rows, feat).astype(jnp.float32)
    a_col[...] = jnp.broadcast_to(scale * jnp.sum(wide * wide, axis=1, keepdims=True), (rows, LANES))
    for g in range(groups):
        span = pl.ds(g * LANES, LANES)
        aq[own_blk, g:g + 1, :] = jnp.transpose(a_col[span, :])[0:1, :]
        aq[own_blk, groups + g:groups + g + 1, :] = q_ref[g:g + 1, :]

    aq_send_if(z > 0, DOWN, own_blk)
    aq_send_if(z < 3, UP, own_blk)
    aq_send_to(SIDE, own_blk)
    aq_send_to(TWIN, own_blk)
    for k in range(1, PARTS):
        send_own(k)
    for g in range(groups):
        q_col[pl.ds(g * LANES, LANES), :] = jnp.transpose(jnp.broadcast_to(q_ref[g:g + 1, :], (LANES, LANES)))
    force[...] = jnp.zeros_like(force)
    row_sum[...] = jnp.zeros_like(row_sum)
    e_acc[...] = jnp.zeros_like(e_acc)

    def share(ch):
        z_j = block_of(ch) % 4
        at_corner = jnp.where(z_j == z, 0.5, 0.0)
        at_middle = jnp.where((z_j == 1) | (z_j == 2), 0.5, 1.0)
        return jnp.where(corner, at_corner, at_middle)

    def weights_of(x_i, a_i, q_i, ch, k):
        blk = block_of(ch)
        def lanes(first):
            return jnp.concatenate([aq[blk, pl.ds(first + h, 1), :] for h in range(2)], axis=1)
        a_i, q_i = (jnp.concatenate([v] * 2, axis=1) for v in (a_i, q_i))
        dots = lax.dot_general(x_i, xs[ch], NT, preferred_element_type=jnp.float32)
        power = jnp.minimum((2.0 * scale * dots - lanes(2 * k)) - a_i, 0.0)
        return (q_i * lanes(groups + 2 * k)) * jnp.exp2(power)

    def fold(weights):
        return weights[:, :LANES] + weights[:, LANES:]

    def stack(halves):
        return jnp.sum(halves.reshape(halves.shape[0] // 8, 8, LANES), axis=0)

    def pairs(chunks, parts_of, masked=False, counted=True):
        x_own = xs[pl.ds(own, PARTS)].reshape(rows, feat)
        total = row_sum[...]
        e_part = jnp.zeros((8, LANES), jnp.float32)
        for n, (ch, k) in enumerate(zip(chunks, parts_of)):
            weights = weights_of(x_own, a_col[...], q_col[...], ch, k)
            if masked:
                rid = lax.broadcasted_iota(jnp.int32, weights.shape, 0)
                cid = lax.broadcasted_iota(jnp.int32, weights.shape, 1)
                weights = jnp.where(rid == cid + n * part, 0.0, weights)
            halves = fold(weights)
            total = total + halves
            if counted:
                part_of_e = share(ch)
                e_part = e_part + jnp.where(part_of_e > 0.0, part_of_e * stack(halves), 0.0)
            low[:, pl.ds(n * part, part)] = weights.astype(jnp.bfloat16)
        row_sum[...] = total
        if counted:
            e_acc[...] += e_part
        acc = force[...]
        for n, ch in enumerate(chunks):
            acc = acc + jnp.dot(low[:, pl.ds(n * part, part)], xs[ch], preferred_element_type=jnp.float32)
        force[...] = acc

    end_rows = chunk(y, far, 0)
    end_cols = [chunk(yy, other, 0) + jnp.where(z == 1, 0, plane) for yy in (y, 1 - y)]

    def end_vectors():
        blk = block_of(end_rows)
        for g in range(groups):
            for ref, first in ((a_end, 0), (q_end, groups)):
                row = aq[blk, first + g:first + g + 1, :]
                ref[pl.ds(g * LANES, LANES), :] = jnp.transpose(jnp.broadcast_to(row, (LANES, LANES)))

    def end_energy(k):
        e_part = jnp.zeros((8, LANES), jnp.float32)
        x_end = xs[pl.ds(end_rows, PARTS)].reshape(rows, feat)
        for cols in end_cols:
            e_part = e_part + stack(fold(weights_of(x_end, a_end[...], q_end[...], cols + k, k)))
        e_acc[...] += e_part

    pairs([own + k for k in range(PARTS)], range(PARTS), masked=True)
    aq_arrive(own_blk + plane // PARTS)
    for k in range(PARTS):
        arrive(own + plane + k)
    pairs([own + plane + k for k in range(2)], range(2))

    place = seg * 4 + z

    def send_energy():
        for d in range(1, 16):
            peer = (place + d) % 16
            pltpu.make_async_remote_copy(
                src_ref=es.at[place], dst_ref=es.at[place], send_sem=e_send, recv_sem=e_recv,
                device_id={'seg': peer // 4, 'col': peer % 4}, device_id_type=MESH).start()

    def cross_event(zb, k, pass_on):
        ch = chunk(1 - y, zb, k)
        arrive(ch)
        if pass_on:
            onward(zb, ch)
        send(TWIN, ch)

    def schedule(u):
        k4 = u % 4
        along_corner = jnp.where(u < 12, chunk(y, line(u // 4), k4), chunk(1 - y, jnp.where(u == 12, near, far), LAST))
        along_middle = jnp.where(u < 8, chunk(y, jnp.where(u < 4, near, far), k4),
                                 jnp.where(u == 8, chunk(1 - y, near, 2), chunk(1 - y, far, u - 9)))
        side_corner = jnp.where(u < 7, chunk(1 - y, near, u - 4),
                                jnp.where(u < 11, chunk(1 - y, other, u - 7), chunk(1 - y, far, u - 11)))
        side_middle = jnp.where(
            u < 8, chunk(1 - y, jnp.where(u % 2 == 0, near, other), u // 2 - 2),
            jnp.where(u < 10, chunk(1 - y, other, u - 6), chunk(1 - y, jnp.where(u == 10, near, far), LAST)))
        side = jnp.where(u < 4, chunk(1 - y, z, u), jnp.where(corner, side_corner, side_middle))
        return jnp.where(corner, along_corner, along_middle), side

    def cross_opens(u):
        return (u == 0) | (u == 4) | (corner & ((u == 7) | (u == 11))) | (~corner & ((u == 5) | (u == 9)))

    def evaluate(chunks, counted=True):
        pairs(chunks, [ch % PARTS for ch in chunks], counted=counted)

    def from_twin(u):
        along, side = (ch + plane for ch in schedule(u))

        @pl.when((u == 0) | (u == 4) | (corner & (u == 8)))
        def _():
            aq_arrive(block_of(along))

        @pl.when(cross_opens(u))
        def _():
            aq_arrive(block_of(jnp.where(~corner & (u == 9), along, side)))

        arrive(along)
        arrive(side)

    def step(u, carry):
        along, side = schedule(u)

        @pl.when(corner)
        def _():
            line_event(line(u // 4), u % 4)

        @pl.when(~corner & (u < 4))
        def _():
            line_event(near, u)
            line_event(other, u)

        @pl.when(~corner & (u >= 4) & (u < 8))
        def _():
            line_event(far, u - 4)

        @pl.when(~corner & (u == 7))
        def _():
            ch = chunk(1 - y, z, LAST)
            send_if(z == 1, DOWN, ch)
            send_if(z == 2, UP, ch)

        @pl.when(~corner & ((u == 6) | (u == 7)))
        def _():
            cross_event(other, u - 4, True)

        @pl.when(~corner & (u == 9))
        def _():
            cross_event(near, LAST, False)

        @pl.when(~corner & (u == 11))
        def _():
            cross_event(far, 2, False)

        @pl.when(corner | (u < 11))
        def _():
            ch = jnp.where(~corner & (u >= 8), along, side)
            arrive(ch)
            send(TWIN, ch)

        @pl.when(~corner & (u == 10))
        def _():
            cross_event(far, LAST, True)

        @pl.when((u == 3) | (corner & (u == 2)))
        def _():
            send_if(z < 2, UP, side)
            send_if(z >= 2, DOWN, side)

        @pl.when(cross_opens(u))
        def _():
            blk = block_of(jnp.where(~corner & (u == 9), along, side))
            aq_arrive(blk)
            aq_send_to(TWIN, blk)

        @pl.when(u > 0)
        def _():
            from_twin(u - 1)

        before = schedule(jnp.maximum(u - 1, 0))
        evaluate([along, side] + [jnp.where(u > 0, ch, own + 2 + n) + plane for n, ch in enumerate(before)])

        @pl.when(~corner & ((u == 1) | (u == 3)))
        def _():
            pair = [chunk(y, other, u - 1), chunk(y, other, u)]

            @pl.when(u == 1)
            def _():
                aq_arrive(block_of(pair[0] + plane))

            for ch in pair:
                arrive(ch + plane)
            evaluate(pair + [ch + plane for ch in pair])

        @pl.when(corner & (u == 6))
        def _():
            es[place] = e_acc[...]

        pl.when(corner & (u == 8))(send_energy)
        pl.when(~corner & (u == 6))(end_vectors)
        pl.when(~corner & (u >= 7) & (u < 11))(lambda: end_energy(u - 7))
        return carry

    lax.fori_loop(0, 12, step, 0)

    def last_steps(i, carry):
        @pl.when(~corner & (i == 1))
        def _():
            es[place] = e_acc[...]

        @pl.when(corner & (i > 0))
        def _():
            cross_event(jnp.where(i == 1, near, far), LAST, False)
            side = schedule(11 + i)[1]
            arrive(side)
            send(TWIN, side)

        pl.when(~corner & (i == 1))(send_energy)

        @pl.when(i == 0)
        def _():
            from_twin(11)
            evaluate([ch + plane for ch in schedule(11)])

        @pl.when(corner & (i > 0))
        def _():
            @pl.when(i == 2)
            def _():
                from_twin(12)
                evaluate(list(schedule(13)) + [ch + plane for ch in schedule(12)], counted=False)
                from_twin(13)

            evaluate([ch + jnp.where(i == 1, 0, plane) for ch in schedule(11 + i)], counted=False)

        return carry

    lax.fori_loop(0, 3, last_steps, 0)

    def drain(sem, ref):
        pltpu.make_async_copy(ref, ref, sem).wait()

    drain(send_sem.at[TWIN], xs.at[pl.ds(0, 8 * PARTS)])

    inv_len2 = 1.0 / feat
    for r in range(PARTS):
        span = pl.ds(r * part, part)
        full = jnp.sum(row_sum[span, :], axis=1, keepdims=True)
        out_ref[span, :] = (full * xs[own + r].astype(jnp.float32) - force[span, :]) * inv_len2

    drain(aq_send.at[TWIN], aq.at[pl.ds(0, 8)])
    drain(aq_send.at[SIDE], aq.at[pl.ds(0, 4)])
    for zz, counts in enumerate(((0, 6, 14), (14, 11, 11), (11, 14, 11), (6, 0, 14))):
        @pl.when(z == zz)
        def _():
            for way, count in zip((DOWN, UP, SIDE), counts):
                if count:
                    drain(send_sem.at[way], xs.at[pl.ds(0, count)])
            if zz:
                drain(aq_send.at[DOWN], aq.at[pl.ds(0, 4 - zz)])
            if zz < 3:
                drain(aq_send.at[UP], aq.at[pl.ds(0, zz + 1)])
    drain(e_recv, es.at[pl.ds(0, 15)])
    drain(e_send, es.at[pl.ds(0, 15)])
    e_ref[0] = jnp.sum(es[...])


def solution(mesh):
    assert (mesh.shape['seg'], mesh.shape['col']) == (4, 4)

    def per_device(x_own, q_own):
        rows, feat = x_own.shape
        part = rows // PARTS
        groups = rows // LANES
        f32, bf16 = jnp.float32, jnp.bfloat16
        vmem = pltpu.VMEM
        dma = pltpu.SemaphoreType.DMA
        return pl.pallas_call(
            pair_kernel,
            out_shape=(jax.ShapeDtypeStruct((rows, feat), f32), jax.ShapeDtypeStruct((1,), f32)),
            in_specs=[pl.BlockSpec(memory_space=pltpu.HBM)] * 2,
            out_specs=(pl.BlockSpec(memory_space=vmem), pl.BlockSpec(memory_space=pltpu.SMEM)),
            scratch_shapes=[
                vmem((16 * PARTS, part, feat), bf16), vmem((16, 2 * groups, LANES), f32), vmem((16, 8, LANES), f32),
                vmem((8, LANES), f32), vmem((groups, LANES), f32),
                vmem((rows, LANES), f32), vmem((rows, LANES), f32), vmem((rows, LANES), f32), vmem((rows, LANES), f32),
                vmem((rows, feat), f32), vmem((rows, LANES), f32), vmem((rows, rows), bf16),
                dma((PARTS + 1,)), dma((16 * PARTS,)), dma((16,)), dma, dma((4,)), dma((4,)), dma],
            compiler_params=pltpu.CompilerParams(
                collective_id=0, has_side_effects=True, vmem_limit_bytes=40 * 2 ** 20),
        )(*(pltpu.with_memory_space_constraint(v, pltpu.HBM) for v in (x_own, q_own.reshape(groups, LANES))))

    row_spec = P(ROW_AXES, None)
    return jax.shard_map(per_device, mesh=mesh, in_specs=(row_spec, P(ROW_AXES)),
                         out_specs=(row_spec, P('sys')), check_vma=False)
```
